64 devices in a mesh: dp: 4 (over x, y), seq: 16 (over z, core).
Axes of the slice: x: 2, y: 2, z: 8, core: 2. Of those that a mesh axis runs over, the one named last changes fastest.
The devices are a block of a 4x4x8 slice.
Arguments:
- enc_out: bfloat16 [64, 384, 1024], P('dp', 'seq'), parts along dimension 0
- pred_out: bfloat16 [64, 24, 320], P('dp'), parts along dimension 0
- w_enc: bfloat16 [1024, 512], replicated
- w_pred: bfloat16 [320, 512], replicated
- w_out: bfloat16 [512, 1024], replicated
- b_out: float32 [1024], replicated
- labels: int32 [64, 23], P('dp'), parts along dimension 0
- frame_len: int32 [64], P('dp'), parts along dimension 0
- label_len: int32 [64], P('dp'), parts along dimension 0
Outputs:
- output: float32 [64], P('dp'), parts along dimension 0
There are 4 independent parts. The reference program is written for one: setup_inputs(seed, part) draws one part's arguments, and reference() takes and returns one part's arrays. A program takes and returns all parts, laid end to end along the dimension named above; an argument that names none is the same for every part.
All inputs are finite; a program needn't handle non-finite values.
Results may differ from the reference program's by a relative error of at most 0.001.
Values are sent between devices in bfloat16 or wider.
A program may use at most 768 MiB of HBM per device.

```python
import math
import jax
import jax.numpy as jnp
from jax import lax

BATCH = 16
FRAMES = 384
PRED_LEN = 24
ENC_DIM = 1024
PRED_DIM = 320
JOINT = 512
VOCAB = 1024

MAX_LABELS = PRED_LEN - 1
NEG_FILL = -1.0e30


def draw_lengths(int_key):
    sub_keys = jax.random.split(int_key, 5)
    labels = jax.random.randint(sub_keys[0], (BATCH, MAX_LABELS), 1, VOCAB, dtype=jnp.int32)
    utt_ids = jnp.arange(BATCH)
    frame_len = jax.random.randint(sub_keys[1], (BATCH,), FRAMES // 4, FRAMES + 1, dtype=jnp.int32)
    frame_pick = jax.random.randint(sub_keys[2], (), 0, BATCH)
    frame_len = jnp.where(utt_ids == frame_pick, FRAMES, frame_len).astype(jnp.int32)
    label_len = jax.random.randint(sub_keys[3], (BATCH,), 1, MAX_LABELS + 1, dtype=jnp.int32)
    label_pick = jax.random.randint(sub_keys[4], (), 0, BATCH)
    label_len = jnp.where(utt_ids == label_pick, MAX_LABELS, label_len).astype(jnp.int32)
    return labels, frame_len, label_len


def setup_inputs(seed: int = 0, part: int = 0) -> dict:
    part_key = jax.random.fold_in(jax.random.key(seed), part)
    val_keys = jax.random.split(part_key, 5)
    shared_keys = jax.random.split(jax.random.key(seed + 1), 5)
    enc_noise = jax.random.normal(val_keys[0], (BATCH, FRAMES, ENC_DIM), jnp.float32)
    enc_mean = jax.random.normal(val_keys[1], (BATCH, 1, ENC_DIM), jnp.float32)
    enc_scale = jax.random.uniform(val_keys[2], (BATCH, 1, 1), jnp.float32, 0.5, 1.5)
    enc_out = (0.8 * enc_scale * (enc_noise + enc_mean)).astype(jnp.bfloat16)
    pred_noise = jax.random.normal(val_keys[3], (BATCH, PRED_LEN, PRED_DIM), jnp.float32)
    pred_mean = jax.random.normal(val_keys[4], (BATCH, 1, PRED_DIM), jnp.float32)
    pred_out = (0.8 * (pred_noise + pred_mean)).astype(jnp.bfloat16)
    w_enc = (jax.random.normal(shared_keys[0], (ENC_DIM, JOINT), jnp.float32) * ENC_DIM ** -0.5).astype(jnp.bfloat16)
    w_pred = (jax.random.normal(shared_keys[1], (PRED_DIM, JOINT), jnp.float32) * PRED_DIM ** -0.5).astype(jnp.bfloat16)
    w_out = (jax.random.normal(shared_keys[2], (JOINT, VOCAB), jnp.float32) * (2.0 * JOINT ** -0.5)).astype(jnp.bfloat16)
    b_rest = 2.5 * jax.random.normal(shared_keys[3], (VOCAB,), jnp.float32)
    b_blank = math.log(VOCAB) + 4.0 + jax.random.uniform(shared_keys[4], (), jnp.float32, -1.0, 1.0)
    b_out = jnp.where(jnp.arange(VOCAB) == 0, b_blank, b_rest).astype(jnp.float32)
    labels, frame_len, label_len = draw_lengths(jax.random.fold_in(part_key, 3))
    return {"enc_out": enc_out, "pred_out": pred_out, "w_enc": w_enc, "w_pred": w_pred, "w_out": w_out, "b_out": b_out, "labels": labels, "frame_len": frame_len, "label_len": label_len}


def reference(enc_out, pred_out, w_enc, w_pred, w_out, b_out, labels, frame_len, label_len):
    enc_proj = jnp.dot(enc_out.reshape(BATCH * FRAMES, ENC_DIM), w_enc, preferred_element_type=jnp.float32)
    enc_proj = enc_proj.astype(jnp.bfloat16).reshape(BATCH, FRAMES, JOINT)
    pred_proj = jnp.dot(pred_out.reshape(BATCH * PRED_LEN, PRED_DIM), w_pred, preferred_element_type=jnp.float32)
    pred_f32 = pred_proj.astype(jnp.bfloat16).astype(jnp.float32).reshape(BATCH, PRED_LEN, JOINT)
    positions = jnp.arange(PRED_LEN)
    end_pos = positions[None, :] == label_len[:, None]
    start_row = jnp.broadcast_to(jnp.where(positions == 0, 0.0, NEG_FILL), (BATCH, PRED_LEN)).astype(jnp.float32)
    zero_col = jnp.zeros((BATCH, 1), jnp.float32)

    def frame_step(carry, step_in):
        row_prev, picked = carry
        enc_row, frame_idx = step_in
        hidden = jnp.tanh(enc_row.astype(jnp.float32)[:, None, :] + pred_f32).astype(jnp.bfloat16)
        logits = jnp.dot(hidden.reshape(BATCH * PRED_LEN, JOINT), w_out, preferred_element_type=jnp.float32)
        log_probs = jax.nn.log_softmax(logits.reshape(BATCH, PRED_LEN, VOCAB) + b_out, axis=-1)
        blank_lp = log_probs[:, :, 0]
        label_lp = jnp.take_along_axis(log_probs[:, :MAX_LABELS, :], labels[:, :, None], axis=2)[:, :, 0]
        cum_label = jnp.concatenate([zero_col, jnp.cumsum(label_lp, axis=1)], axis=1)
        row_next = cum_label + lax.cumlogsumexp(row_prev - cum_label, axis=1) + blank_lp
        at_end = frame_idx == frame_len - 1
        picked = picked + jnp.where(at_end, jnp.sum(jnp.where(end_pos, row_next, 0.0), axis=1), 0.0)
        return (row_next, picked), None

    scan_init = (start_row, jnp.zeros((BATCH,), jnp.float32))
    (_, picked), _ = lax.scan(frame_step, scan_init, (jnp.swapaxes(enc_proj, 0, 1), jnp.arange(FRAMES)))
    return -picked
```

```python
import functools
import jax
import jax.numpy as jnp
from jax import lax
from jax.experimental import pallas as pl
from jax.experimental.pallas import tpu as pltpu
from jax.sharding import PartitionSpec as P

NEG_FILL = -1.0e30
OCT = 8
ITEMS = 32
GROUP = 32
N_HANDLERS = 4
MESH = pl.DeviceIdType.MESH


def joint_kernel(enc_hbm, pred_hbm, wenc_hbm, wpred_hbm, wout_hbm, bout_ref, lab_ref, flen_ref, llen_ref,
                 blank_out, label_out,
                 enc_v, pred_v, wenc_v, wpred_v, wout_v, w_t, bias_t, a_v, c_v, hid, z_a, z_b, mx_v, o_v,
                 lab_pad, tab_v, tab_s, sems, tab_sem):
    n_utt, n_lab = lab_ref.shape
    n_pos = n_lab + 1
    t_local = enc_v.shape[0] // n_utt
    n_oct = t_local // OCT
    joint, vocab = wout_v.shape
    n_rows = n_utt * GROUP
    t0 = lax.axis_index("seq") * t_local

    copies = [
        pltpu.make_async_copy(src, dst, sems.at[k])
        for k, (src, dst) in enumerate([
            (wout_hbm, wout_v), (enc_hbm, enc_v), (wenc_hbm, wenc_v), (pred_hbm, pred_v), (wpred_hbm, wpred_v)])
    ]
    for copy in copies:
        copy.start()

    lab_pad[...] = jnp.zeros_like(lab_pad)
    lab_pad[:, :n_lab] = lab_ref[...]
    tab_rows = tab_v.shape[1]
    shape = (tab_rows, 128)
    cums, total = [], jnp.int32(0)
    lens, nus = [], []
    for b in range(n_utt):
        n_t = jnp.clip((flen_ref[b] - t0 + OCT - 1) // OCT, 0, n_oct)
        nu = llen_ref[b] + 1
        cums.append(total)
        nus.append(nu)
        total = total + n_t * nu
    item = lax.broadcasted_iota(jnp.int32, shape, 0) * 128 + lax.broadcasted_iota(jnp.int32, shape, 1)
    item = jnp.minimum(item, total - 1)
    utt = jnp.zeros(shape, jnp.int32)
    base = jnp.zeros(shape, jnp.int32)
    width = jnp.ones(shape, jnp.int32)
    for b in range(n_utt):
        hit = item >= cums[b]
        utt = jnp.where(hit, b, utt)
        base = jnp.where(hit, cums[b], base)
        width = jnp.where(hit, nus[b], width)
    rest = item - base
    octet = jnp.zeros(shape, jnp.int32)
    for k in range(1, n_oct):
        octet = octet + jnp.where(rest >= k * width, 1, 0)
    pos = jnp.clip(rest - octet * width, 0, n_pos - 1)
    word = jnp.zeros(shape, jnp.int32)
    for b in range(n_utt):
        row = jnp.broadcast_to(lab_pad[b:b + 1, :], shape)
        word = jnp.where(utt == b, jnp.take_along_axis(row, pos, axis=1, mode="promise_in_bounds"), word)
    tab_v[0] = (utt * t_local + octet * OCT) + (utt * n_pos + pos) * 65536
    tab_v[1] = word + (octet * n_rows + utt * GROUP + pos) * 65536
    tab_copy = pltpu.make_async_copy(tab_v, tab_s, tab_sem)
    tab_copy.start()

    copies[0].wait()
    for k in range(vocab // 128):
        cols = pl.ds(k * 128, 128)
        w_t[cols, :] = wout_v[:, cols].T
        bias_t[cols, :] = jnp.broadcast_to(bout_ref[k:k + 1, :], (128, 128)).T
    copies[1].wait()
    copies[2].wait()
    a_v[...] = jnp.dot(enc_v[...], wenc_v[...], preferred_element_type=jnp.float32).astype(jnp.bfloat16).astype(jnp.float32)
    copies[3].wait()
    copies[4].wait()
    c_v[...] = jnp.dot(pred_v[...], wpred_v[...], preferred_element_type=jnp.float32).astype(jnp.bfloat16).astype(jnp.float32)
    tab_copy.wait()

    lane16 = lax.broadcasted_iota(jnp.int32, (16, 128), 1)
    spread_idx = lax.broadcasted_iota(jnp.int32, (16, 128), 0) * OCT + lane16 % OCT
    is_blank = lane16 % 16 < OCT
    lane_item = lax.broadcasted_iota(jnp.int32, (1, 128), 1) // OCT

    def fields(which, k):
        both = tab_s[which, k // 128, k % 128]
        return both & 65535, both >> 16

    def make_hidden(tile):
        for q in range(ITEMS // 2):
            parts = []
            for k in (2 * q, 2 * q + 1):
                a_row, c_row = fields(0, tile * ITEMS + k)
                parts.append(a_v[pl.ds(pl.multiple_of(a_row, OCT), OCT), :] + c_v[pl.ds(c_row, 1), :])
            hid[16 * q:16 * q + 16, :] = jnp.tanh(jnp.concatenate(parts, axis=0)).astype(jnp.bfloat16)

    def finish(tile):
        labs = [fields(1, tile * ITEMS + k) for k in range(ITEMS)]
        lab_z = []
        for g in range(2):
            acc = jnp.zeros((1, 128), jnp.float32)
            for k in range(16):
                z_row = (z_a, z_b)[g][pl.ds(labs[16 * g + k][0], 1), :]
                acc = jnp.where(lane_item == k, z_row, acc)
            lab_z.append(acc)
        blank_z = jnp.concatenate([z_a[0:1, :], z_b[0:1, :]], axis=1)
        mx = jnp.max(mx_v[...], axis=0, keepdims=True)
        part = jnp.zeros((8, 256), jnp.float32)
        for k in range(vocab // 128):
            rows = slice(k * 128, k * 128 + 128)
            z = jnp.concatenate([z_a[rows, :], z_b[rows, :]], axis=1)
            part = part + jnp.sum(jnp.exp(z - mx).reshape(16, 8, 256), axis=0)
        lse = mx + jnp.log(jnp.sum(part, axis=0, keepdims=True))
        for g in range(2):
            lanes = slice(128 * g, 128 * g + 128)
            blank_lp = jnp.broadcast_to(blank_z[:, lanes] - lse[:, lanes], (16, 128))
            label_lp = jnp.broadcast_to(lab_z[g] - lse[:, lanes], (16, 128))
            wide = jnp.where(is_blank, jnp.take_along_axis(blank_lp, spread_idx, axis=1, mode="promise_in_bounds"),
                             jnp.take_along_axis(label_lp, spread_idx, axis=1, mode="promise_in_bounds"))
            for k in range(16):
                o_v[pl.ds(labs[16 * g + k][1], 1), :] = wide[k:k + 1, :]

    def matmul():
        z = lax.dot_general(w_t[...], hid[...], (((1,), (1,)), ((), ())), preferred_element_type=jnp.float32)
        bias = bias_t[...]
        z = z + jnp.concatenate([bias, bias], axis=1)
        z_a[...] = z[:, :128]
        z_b[...] = z[:, 128:]
        mx_v[...] = jnp.max(z.reshape(vocab // 8, 8, 256), axis=0)

    n_tiles = (total + ITEMS - 1) // ITEMS

    @pl.when(n_tiles > 0)
    def _():
        make_hidden(0)
        matmul()
        make_hidden(jnp.minimum(1, n_tiles - 1))

        def step(i, _):
            finish(i - 1)
            matmul()
            make_hidden(jnp.minimum(i + 1, n_tiles - 1))
            return 0

        lax.fori_loop(1, n_tiles, step, 0)
        finish(n_tiles - 1)

    lane_b = lax.broadcasted_iota(jnp.int32, (1, n_rows), 1) // GROUP
    lane_u = lax.broadcasted_iota(jnp.int32, (1, n_rows), 1) % GROUP
    flen = jnp.zeros((1, n_rows), jnp.int32)
    llen = jnp.zeros((1, n_rows), jnp.int32)
    for b in range(n_utt):
        flen = jnp.where(lane_b == b, flen_ref[b], flen)
        llen = jnp.where(lane_b == b, llen_ref[b], llen)
    lane128 = lax.broadcasted_iota(jnp.int32, (128, 128), 1)
    frame8 = lax.broadcasted_iota(jnp.int32, (OCT, 128), 0)
    for r in range(n_rows // 128):
        merged = o_v[128 * r:128 * r + 128, :]
        for k in range(1, n_oct):
            merged = jnp.where(lane128 >= 16 * k, o_v[k * n_rows + 128 * r:k * n_rows + 128 * r + 128, :], merged)
        turned = merged.T
        lanes = slice(128 * r, 128 * r + 128)
        for k in range(n_oct):
            live = (t0 + k * OCT + frame8 < flen[:, lanes]) & (lane_u[:, lanes] <= llen[:, lanes])
            live_lab = live & (lane_u[:, lanes] < llen[:, lanes])
            blank_out[k * OCT:k * OCT + OCT, lanes] = jnp.where(live, turned[16 * k:16 * k + 8, :], 0.0)
            label_out[k * OCT:k * OCT + OCT, lanes] = jnp.where(live_lab, turned[16 * k + 8:16 * k + 16, :], NEG_FILL)


def log_add(x, y):
    return jnp.maximum(x, y) + jnp.log(1.0 + jnp.exp(-jnp.abs(x - y)))


def lattice_kernel(n_seq, blank_ref, label_ref, llen_ref, loss_ref,
                   blank_s, label_s, m_loc, m_recv, v_out, v_recv, send_sem, recv_sem, out_sem, in_sem):
    t_local, n_rows = blank_ref.shape
    n_pos = m_loc.shape[1]
    me = lax.axis_index("seq")
    first_handler = n_seq - N_HANDLERS
    mine = me >= first_handler
    my_hand = jnp.maximum(me - first_handler, 0)

    barrier = pltpu.get_barrier_semaphore()
    for k in range(1, n_seq):
        other = lax.rem(me + k, n_seq)

        @pl.when(mine | (other >= first_handler))
        def _():
            pl.semaphore_signal(barrier, inc=1, device_id={"seq": other}, device_id_type=MESH)

    n_skew = blank_s.shape[0]
    lane_u = lax.broadcasted_iota(jnp.int32, (n_skew, n_rows), 1) % GROUP
    fills = ((blank_ref, blank_s, 0.0), (label_ref, label_s, NEG_FILL))
    for src, dst, fill in fills:
        rows = jnp.concatenate([src[...], jnp.full((n_skew - t_local, n_rows), fill, jnp.float32)], axis=0)
        for bit in (1, 2, 4, 8, 16):
            rows = jnp.where((lane_u & bit) != 0, pltpu.roll(rows, bit, 0), rows)
        dst[...] = rows

    shape = (n_pos, n_rows)
    start = jnp.where(lax.broadcasted_iota(jnp.int32, shape, 0) == lax.broadcasted_iota(jnp.int32, shape, 1) % GROUP,
                      0.0, NEG_FILL)

    def diagonal(d, carry):
        stay, move = carry
        alpha = log_add(stay, pltpu.roll(move, 1, 1))
        return alpha + blank_s[pl.ds(d, 1), :], alpha + label_s[pl.ds(d, 1), :]

    stay, _ = lax.fori_loop(0, t_local + n_pos - 1, diagonal, (start, jnp.full(shape, NEG_FILL, jnp.float32)))
    for h in range(N_HANDLERS):
        m_loc[h] = stay[:, 128 * h:128 * h + 128]

    pl.semaphore_wait(barrier, jnp.where(mine, n_seq - 1, N_HANDLERS))

    def send_matrix(h):
        return pltpu.make_async_remote_copy(
            src_ref=m_loc.at[h], dst_ref=m_recv.at[me], send_sem=send_sem.at[h], recv_sem=recv_sem.at[me],
            device_id={"seq": first_handler + h}, device_id_type=MESH)

    for h in range(N_HANDLERS):
        @pl.when(me != first_handler + h)
        def _():
            send_matrix(h).start()

        @pl.when(me == first_handler + h)
        def _():
            m_recv[me] = m_loc[h]

    def send_row(k):
        return pltpu.make_async_remote_copy(
            src_ref=v_out, dst_ref=v_recv.at[my_hand], send_sem=out_sem.at[k], recv_sem=in_sem.at[my_hand],
            device_id={"seq": lax.rem(me + k, n_seq)}, device_id_type=MESH)

    @pl.when(mine)
    def _():
        def arrived(src):
            @pl.when(src != me)
            def _():
                pltpu.make_async_remote_copy(
                    src_ref=m_loc.at[0], dst_ref=m_recv.at[src], send_sem=send_sem.at[0], recv_sem=recv_sem.at[src],
                    device_id={"seq": src}, device_id_type=MESH).wait_recv()

        sub = lax.broadcasted_iota(jnp.int32, (n_pos, 128), 0)
        lane = lax.broadcasted_iota(jnp.int32, (n_pos, 128), 1)
        turn_idx = lane // GROUP * GROUP + sub

        def join(src, row):
            arrived(src)
            col = jnp.take_along_axis(jnp.broadcast_to(row, (n_pos, 128)), turn_idx, axis=1, mode="promise_in_bounds")
            terms = col + m_recv[src]
            top = jnp.max(terms, axis=0, keepdims=True)
            return top + jnp.log(jnp.sum(jnp.exp(terms - top), axis=0, keepdims=True))

        arrived(jnp.int32(0))
        row = m_recv[0, 0:1, :]
        row = lax.fori_loop(1, n_seq, join, row)
        sub8 = lax.broadcasted_iota(jnp.int32, (8, 128), 0)
        lane8 = lax.broadcasted_iota(jnp.int32, (8, 128), 1)
        want = jnp.full((8, 128), -1, jnp.int32)
        for b in range(llen_ref.shape[0]):
            want = jnp.where((my_hand * (128 // GROUP) + sub8) == b, llen_ref[b], want)
        keep = (lane8 // GROUP == sub8) & (lane8 % GROUP == want)
        column = jnp.sum(jnp.where(keep, row, 0.0), axis=1, keepdims=True)
        here = (lane8 == my_hand * (128 // GROUP) + sub8) & (sub8 < 128 // GROUP)
        v_out[...] = jnp.broadcast_to(jnp.sum(jnp.where(here, column, 0.0), axis=0, keepdims=True), (8, 128))
        for k in range(1, n_seq):
            send_row(k).start()
        v_recv[my_hand] = v_out[...]

    total = jnp.zeros((1, 128), jnp.float32)
    for h in range(N_HANDLERS):
        @pl.when(me != first_handler + h)
        def _():
            pltpu.make_async_remote_copy(
                src_ref=v_out, dst_ref=v_recv.at[h], send_sem=out_sem.at[0], recv_sem=in_sem.at[h],
                device_id={"seq": first_handler + h}, device_id_type=MESH).wait_recv()
    for h in range(N_HANDLERS):
        total = total + v_recv[h, 0:1, :]
    loss_ref[...] = -total[:, :loss_ref.shape[1]]

    for h in range(N_HANDLERS):
        @pl.when(me != first_handler + h)
        def _():
            send_matrix(h).wait_send()

    @pl.when(mine)
    def _():
        for k in range(1, n_seq):
            send_row(k).wait_send()


def solution(mesh):
    n_seq = mesh.shape["seq"]

    def local_loss(enc_blk, pred_out, w_enc, w_pred, w_out, b_out, labels, frame_len, label_len):
        n_utt, t_local, d_enc = enc_blk.shape
        n_pos, d_pred = pred_out.shape[1:]
        joint, vocab = w_out.shape
        n_rows = n_utt * GROUP
        n_oct = t_local // OCT
        max_items = n_utt * n_pos * n_oct
        tab_rows = -(-(max_items + ITEMS) // 1024) * 8
        hbm = pl.BlockSpec(memory_space=pl.ANY)
        vmem = pl.BlockSpec(memory_space=pltpu.VMEM)
        smem = pl.BlockSpec(memory_space=pltpu.SMEM)
        f32, bf16 = jnp.float32, jnp.bfloat16
        lattice_shape = jax.ShapeDtypeStruct((t_local, n_rows), f32)
        blank, label = pl.pallas_call(
            joint_kernel,
            out_shape=(lattice_shape, lattice_shape),
            in_specs=[hbm] * 5 + [vmem, vmem, smem, smem],
            out_specs=(vmem, vmem),
            scratch_shapes=[
                pltpu.VMEM((n_utt * t_local, d_enc), bf16),
                pltpu.VMEM((n_utt * n_pos, d_pred), bf16),
                pltpu.VMEM((d_enc, joint), bf16),
                pltpu.VMEM((d_pred, joint), bf16),
                pltpu.VMEM((joint, vocab), bf16),
                pltpu.VMEM((vocab, joint), bf16),
                pltpu.VMEM((vocab, 128), f32),
                pltpu.VMEM((n_utt * t_local, joint), f32),
                pltpu.VMEM((n_utt * n_pos, joint), f32),
                pltpu.VMEM((ITEMS * OCT, joint), bf16),
                pltpu.VMEM((vocab, 128), f32),
                pltpu.VMEM((vocab, 128), f32),
                pltpu.VMEM((8, ITEMS * OCT), f32),
                pltpu.VMEM((n_oct * n_rows, 128), f32),
                pltpu.VMEM((n_utt, 128), jnp.int32),
                pltpu.VMEM((2, tab_rows, 128), jnp.int32),
                pltpu.SMEM((2, tab_rows, 128), jnp.int32),
                pltpu.SemaphoreType.DMA((5,)),
                pltpu.SemaphoreType.DMA,
            ],
            name="joint",
        )(enc_blk.reshape(n_utt * t_local, d_enc), pred_out.reshape(n_utt * n_pos, d_pred), w_enc, w_pred, w_out,
          b_out.reshape(vocab // 128, 128), labels, frame_len, label_len)

        loss = pl.pallas_call(
            functools.partial(lattice_kernel, n_seq),
            out_shape=jax.ShapeDtypeStruct((1, n_utt), f32),
            in_specs=[vmem, vmem, smem],
            out_specs=vmem,
            scratch_shapes=[
                pltpu.VMEM((t_local + n_pos, n_rows), f32),
                pltpu.VMEM((t_local + n_pos, n_rows), f32),
                pltpu.VMEM((N_HANDLERS, n_pos, 128), f32),
                pltpu.VMEM((n_seq, n_pos, 128), f32),
                pltpu.VMEM((8, 128), f32),
                pltpu.VMEM((N_HANDLERS, 8, 128), f32),
                pltpu.SemaphoreType.DMA((N_HANDLERS,)),
                pltpu.SemaphoreType.DMA((n_seq,)),
                pltpu.SemaphoreType.DMA((n_seq,)),
                pltpu.SemaphoreType.DMA((N_HANDLERS,)),
            ],
            compiler_params=pltpu.CompilerParams(collective_id=0, has_side_effects=True),
            name="lattice",
        )(blank, label, label_len)
        return loss.reshape(n_utt)

    in_specs = (P("dp", "seq", None), P("dp", None, None), P(), P(), P(), P(), P("dp", None), P("dp"), P("dp"))
    return jax.shard_map(local_loss, mesh=mesh, in_specs=in_specs, out_specs=P("dp"), check_vma=False)
```

```python
import functools
import jax
import jax.numpy as jnp
from jax import lax
from jax.experimental import pallas as pl
from jax.experimental.pallas import tpu as pltpu
from jax.sharding import PartitionSpec as P

NEG_FILL = -1.0e30
OCT = 8
ITEMS = 32
GROUP = 32
MESH = pl.DeviceIdType.MESH


def joint_kernel(enc_hbm, pred_hbm, wenc_hbm, wpred_hbm, wout_hbm, bout_hbm, lab_hbm, flen_hbm, llen_hbm,
                 m_out,
                 enc_v, pred_v, wenc_v, wpred_v, wout_v, bout_v, lab_raw, lab_v, flen_s, llen_s,
                 w_t, bias_t, a_v, c_v, hid, z_v, blank_d, label_d, turn_v, tab_v, tab_s, sems, tab_sem):
    n_utt, n_lab = lab_hbm.shape
    n_pos = n_lab + 1
    t_local = enc_v.shape[0] // n_utt
    n_oct = t_local // OCT
    joint, vocab = wout_v.shape
    n_slab = joint // 128
    rep = 128 // n_utt
    t0 = lax.axis_index("seq") * t_local

    copies = [
        pltpu.make_async_copy(src, dst, sems.at[k])
        for k, (src, dst) in enumerate([
            (flen_hbm, flen_s), (llen_hbm, llen_s), (lab_hbm, lab_raw), (bout_hbm, bout_v),
            (wout_hbm, wout_v), (enc_hbm, enc_v), (wenc_hbm, wenc_v), (pred_hbm, pred_v), (wpred_hbm, wpred_v)])
    ]
    for copy in copies:
        copy.start()

    blank_d[...] = jnp.zeros_like(blank_d)
    label_d[...] = jnp.full(label_d.shape, NEG_FILL, jnp.float32)

    for copy in copies[:3]:
        copy.wait()
    lab_v[...] = jnp.zeros_like(lab_v)
    lab_v[:, :n_lab] = lab_raw[...]
    shape = tab_v.shape[1:]
    cums, nus, total = [], [], jnp.int32(0)
    for b in range(n_utt):
        n_t = jnp.clip((flen_s[b] - t0 + OCT - 1) // OCT, 0, n_oct)
        cums.append(total)
        nus.append(llen_s[b] + 1)
        total = total + n_t * nus[b]
    lane = lax.broadcasted_iota(jnp.int32, shape, 1)
    item = lax.broadcasted_iota(jnp.int32, shape, 0) * ITEMS + lane % ITEMS
    item = jnp.minimum(item, total - 1)
    utt = jnp.zeros(shape, jnp.int32)
    base = jnp.zeros(shape, jnp.int32)
    width = jnp.ones(shape, jnp.int32)
    frames = jnp.zeros(shape, jnp.int32)
    for b in range(n_utt):
        hit = item >= cums[b]
        utt = jnp.where(hit, b, utt)
        base = jnp.where(hit, cums[b], base)
        width = jnp.where(hit, nus[b], width)
        frames = jnp.where(hit, flen_s[b] - t0, frames)
    rest = item - base
    octet = jnp.zeros(shape, jnp.int32)
    for k in range(1, n_oct):
        octet = octet + jnp.where(rest >= k * width, 1, 0)
    pos = jnp.clip(rest - octet * width, 0, n_pos - 1)
    word = jnp.zeros(shape, jnp.int32)
    for b in range(n_utt):
        row = jnp.broadcast_to(lab_v[b:b + 1, :], shape)
        word = jnp.where(utt == b, jnp.take_along_axis(row, pos, axis=1, mode="promise_in_bounds"), word)
    has_label = pos < width - 1
    word = jnp.where(has_label, word, 0)
    field = lane // ITEMS
    tab_v[0] = jnp.where(field == 0, utt * t_local + octet * OCT,
                         jnp.where(field == 1, utt * n_pos + pos,
                                   jnp.where(field == 2, word, (octet * n_pos + pos) * OCT)))
    tab_v[1] = jnp.where(field == 0, utt, jnp.where(field == 1, jnp.where(has_label, utt, -1), frames - octet * OCT))
    tab_copy = pltpu.make_async_copy(tab_v, tab_s, tab_sem)
    tab_copy.start()

    copies[3].wait()
    copies[4].wait()
    top_bias = jnp.max(bout_v[...])
    spread = jnp.zeros((8, 128), jnp.float32)
    for k in range(vocab // 128):
        cols = pl.ds(k * 128, 128)
        w_t[cols, :] = wout_v[:, cols].T
        bias_t[cols, :] = jnp.broadcast_to(bout_v[k:k + 1, :] - top_bias, (128, 128)).T
        mass = jnp.sum(jnp.abs(wout_v[:, cols].astype(jnp.float32)).reshape(joint // 8, 8, 128), axis=0)
        spread = jnp.maximum(spread, jnp.sum(mass, axis=0, keepdims=True))
    narrow = jnp.max(spread) <= 60.0
    copies[5].wait()
    copies[6].wait()
    proj = jnp.dot(enc_v[...], wenc_v[...], preferred_element_type=jnp.float32).astype(jnp.bfloat16).astype(jnp.float32)
    for s in range(n_slab):
        a_v[s] = proj[:, 128 * s:128 * s + 128]
    copies[7].wait()
    copies[8].wait()
    proj = jnp.dot(pred_v[...], wpred_v[...], preferred_element_type=jnp.float32).astype(jnp.bfloat16).astype(jnp.float32)
    for s in range(n_slab):
        c_v[s] = proj[:, 128 * s:128 * s + 128]
    tab_copy.wait()

    lane8 = lax.broadcasted_iota(jnp.int32, (OCT, 128), 1)
    frame8 = lax.broadcasted_iota(jnp.int32, (OCT, 128), 0)
    lane_utt = lane8 // rep
    lane_item = lax.broadcasted_iota(jnp.int32, (1, 128), 1) // OCT

    def make_hidden(tile):
        for q in range(ITEMS // 2):
            for s in range(n_slab):
                parts = []
                for k in (2 * q, 2 * q + 1):
                    a_row = pl.multiple_of(tab_s[0, tile, k], OCT)
                    parts.append(a_v[s, pl.ds(a_row, OCT), :] + c_v[s, pl.ds(tab_s[0, tile, ITEMS + k], 1), :])
                hid[16 * q:16 * q + 16, 128 * s:128 * s + 128] = jnp.tanh(
                    jnp.concatenate(parts, axis=0)).astype(jnp.bfloat16)

    def finish(tile, with_max):
        for g in range(2):
            label_z = jnp.zeros((1, 128), jnp.float32)
            for k in range(16):
                y = tab_s[0, tile, 2 * ITEMS + 16 * g + k]
                label_z = jnp.where(lane_item == k, z_v[g, pl.ds(y, 1), :] + bias_t[pl.ds(y, 1), :], label_z)
            blank_z = z_v[g, 0:1, :] + bias_t[0:1, :]
            top = jnp.zeros((1, 128), jnp.float32)
            if with_max:
                part = jnp.full((8, 128), NEG_FILL, jnp.float32)
                for k in range(vocab // 128):
                    rows = slice(k * 128, k * 128 + 128)
                    part = jnp.maximum(part, jnp.max((z_v[g, rows, :] + bias_t[rows, :]).reshape(16, 8, 128), axis=0))
                top = jnp.max(part, axis=0, keepdims=True)
            part = jnp.zeros((8, 128), jnp.float32)
            for k in range(vocab // 128):
                rows = slice(k * 128, k * 128 + 128)
                logit = z_v[g, rows, :] + bias_t[rows, :]
                if with_max:
                    logit = logit - top
                part = part + jnp.sum(jnp.exp(logit).reshape(16, 8, 128), axis=0)
            lse = jnp.log(jnp.sum(part, axis=0, keepdims=True)) + top
            blank_lp = jnp.broadcast_to(blank_z - lse, (OCT, 128))
            label_lp = jnp.broadcast_to(label_z - lse, (OCT, 128))
            for k in range(16):
                j = 16 * g + k
                live = frame8 < tab_s[1, tile, 2 * ITEMS + j]
                row = pl.ds(pl.multiple_of(tab_s[0, tile, 3 * ITEMS + j], OCT), OCT)
                pick = frame8 + OCT * k
                value = jnp.take_along_axis(blank_lp, pick, axis=1, mode="promise_in_bounds")
                pltpu.store(blank_d.at[row, :], value, mask=(lane_utt == tab_s[1, tile, j]) & live)
                value = jnp.take_along_axis(label_lp, pick, axis=1, mode="promise_in_bounds")
                pltpu.store(label_d.at[row, :], value, mask=(lane_utt == tab_s[1, tile, ITEMS + j]) & live)

    def matmul():
        z = lax.dot_general(w_t[...], hid[...], (((1,), (1,)), ((), ())), preferred_element_type=jnp.float32)
        z_v[0] = z[:, :128]
        z_v[1] = z[:, 128:]

    n_tiles = (total + ITEMS - 1) // ITEMS

    def run_tiles(with_max):
        make_hidden(0)
        matmul()
        make_hidden(jnp.minimum(1, n_tiles - 1))

        def step(i, _):
            finish(i - 1, with_max)
            matmul()
            make_hidden(jnp.minimum(i + 1, n_tiles - 1))
            return 0

        lax.fori_loop(1, n_tiles, step, 0)
        finish(n_tiles - 1, with_max)

    @pl.when((n_tiles > 0) & narrow)
    def _():
        run_tiles(False)

    @pl.when((n_tiles > 0) & jnp.logical_not(narrow))
    def _():
        run_tiles(True)

    entry = frame8 * rep + lane8 % rep
    stay = [jnp.where(entry == u, 0.0, NEG_FILL) for u in range(n_pos)]
    move = [None] * n_pos
    for d in range(t_local + n_pos - 1):
        for u in range(min(d, n_pos - 1), max(d - t_local, -1), -1):
            t = d - u
            row = (t // OCT * n_pos + u) * OCT + t % OCT
            if u == 0:
                alpha = stay[0]
            else:
                high, low = jnp.maximum(stay[u], move[u - 1]), jnp.minimum(stay[u], move[u - 1])
                alpha = high + jnp.log(1.0 + jnp.exp(low - high))
            stay[u] = alpha + blank_d[row:row + 1, :]
            move[u] = alpha + label_d[row:row + 1, :]
    for u in range(n_pos):
        for j in range(n_pos // rep):
            turn_v[GROUP * j + u:GROUP * j + u + 1, :] = stay[u][j:j + 1, :]
    turned = turn_v[...].T
    per = 128 // GROUP
    group = lane8 // GROUP
    for h in range(n_utt // per):
        for j in range(n_pos // rep):
            out = None
            for q in range(per):
                b = per * h + q
                piece = turned[rep * b:rep * b + rep, :]
                if q != j:
                    piece = pltpu.roll(piece, (GROUP * (q - j)) % 128, 1)
                out = piece if out is None else jnp.where(group == q, piece, out)
            m_out[h, rep * j:rep * j + rep, :] = out


def lattice_kernel(n_seq, m_hbm, llen_hbm, loss_ref,
                   m_recv, llen_s, v_out, v_recv, send_sem, recv_sem, out_sem, in_sem, own_sem):
    n_hand, n_pos = m_hbm.shape[:2]
    n_utt = llen_hbm.shape[0]
    per = 128 // GROUP
    me = lax.axis_index("seq")
    mine = me < n_hand
    my_hand = jnp.minimum(me, n_hand - 1)

    barrier = pltpu.get_barrier_semaphore()

    def greet(other):
        pl.semaphore_signal(barrier, inc=1, device_id={"seq": other}, device_id_type=MESH)

    for h in range(n_hand):
        @pl.when(me != h)
        def _():
            greet(h)

    @pl.when(mine)
    def _():
        for d in range(n_hand, n_seq):
            greet(d)

    own_len = pltpu.make_async_copy(llen_hbm, llen_s, own_sem.at[0])
    own_matrix = pltpu.make_async_copy(m_hbm.at[my_hand], m_recv.at[me], own_sem.at[1])

    @pl.when(mine)
    def _():
        own_len.start()
        own_matrix.start()

    pl.semaphore_wait(barrier, jnp.where(mine, n_seq - 1, n_hand))

    def send_matrix(h):
        return pltpu.make_async_remote_copy(
            src_ref=m_hbm.at[h], dst_ref=m_recv.at[me], send_sem=send_sem.at[h], recv_sem=recv_sem.at[me],
            device_id={"seq": h}, device_id_type=MESH)

    for h in range(n_hand):
        @pl.when(me != h)
        def _():
            send_matrix(h).start()

    def send_row(d):
        return pltpu.make_async_remote_copy(
            src_ref=v_out, dst_ref=v_recv.at[my_hand], send_sem=out_sem.at[d], recv_sem=in_sem.at[my_hand],
            device_id={"seq": d}, device_id_type=MESH)

    @pl.when(mine)
    def _():
        own_len.wait()
        own_matrix.wait()

        def arrived(src):
            @pl.when(src != me)
            def _():
                pltpu.make_async_remote_copy(
                    src_ref=m_hbm.at[0], dst_ref=m_recv.at[src], send_sem=send_sem.at[0], recv_sem=recv_sem.at[src],
                    device_id={"seq": src}, device_id_type=MESH).wait_recv()

        sub = lax.broadcasted_iota(jnp.int32, (n_pos, 128), 0)
        lane = lax.broadcasted_iota(jnp.int32, (n_pos, 128), 1)
        turn_idx = lane // GROUP * GROUP + sub

        def join(src, row):
            arrived(src)
            col = jnp.take_along_axis(jnp.broadcast_to(row, (n_pos, 128)), turn_idx, axis=1, mode="promise_in_bounds")
            terms = col + m_recv[src]
            top = jnp.max(terms, axis=0, keepdims=True)
            return top + jnp.log(jnp.sum(jnp.exp(terms - top), axis=0, keepdims=True))

        arrived(jnp.int32(0))
        row = m_recv[0, 0:1, :]
        row = lax.fori_loop(1, n_seq, join, row)
        sub8 = lax.broadcasted_iota(jnp.int32, (8, 128), 0)
        lane8 = lax.broadcasted_iota(jnp.int32, (8, 128), 1)
        want = jnp.full((8, 128), -1, jnp.int32)
        for b in range(n_utt):
            want = jnp.where(my_hand * per + sub8 == b, llen_s[b], want)
        keep = (lane8 // GROUP == sub8) & (lane8 % GROUP == want)
        column = jnp.sum(jnp.where(keep, row, 0.0), axis=1, keepdims=True)
        here = (lane8 == my_hand * per + sub8) & (sub8 < per)
        v_out[...] = jnp.sum(jnp.where(here, column, 0.0), axis=0, keepdims=True)
        for d in range(n_seq):
            @pl.when(me != d)
            def _():
                send_row(d).start()
        v_recv[my_hand] = v_out[...]

    for h in range(n_hand):
        @pl.when(me != h)
        def _():
            pltpu.make_async_remote_copy(
                src_ref=v_out, dst_ref=v_recv.at[h], send_sem=out_sem.at[0], recv_sem=in_sem.at[h],
                device_id={"seq": h}, device_id_type=MESH).wait_recv()
    total = v_recv[0]
    for h in range(1, n_hand):
        total = total + v_recv[h]
    loss_ref[...] = -total[0, :n_utt]

    for h in range(n_hand):
        @pl.when(me != h)
        def _():
            send_matrix(h).wait_send()

    @pl.when(mine)
    def _():
        for d in range(n_seq):
            @pl.when(me != d)
            def _():
                send_row(d).wait_send()


def joint_call(enc_blk, pred_out, w_enc, w_pred, w_out, b_out, labels, frame_len, label_len):
    n_utt, t_local, d_enc = enc_blk.shape
    n_pos, d_pred = pred_out.shape[1:]
    joint, vocab = w_out.shape
    n_oct = t_local // OCT
    n_slab = joint // 128
    per = 128 // GROUP
    tab_rows = -(-(n_utt * n_pos * n_oct // ITEMS + 1) // 8) * 8
    hbm = pl.BlockSpec(memory_space=pl.ANY)
    vmem = pl.BlockSpec(memory_space=pltpu.VMEM)
    f32, bf16, i32 = jnp.float32, jnp.bfloat16, jnp.int32
    return pl.pallas_call(
        joint_kernel,
        out_shape=jax.ShapeDtypeStruct((n_utt // per, n_pos, 128), f32),
        in_specs=[hbm] * 9,
        out_specs=vmem,
        scratch_shapes=[
            pltpu.VMEM((n_utt * t_local, d_enc), bf16),
            pltpu.VMEM((n_utt * n_pos, d_pred), bf16),
            pltpu.VMEM((d_enc, joint), bf16),
            pltpu.VMEM((d_pred, joint), bf16),
            pltpu.VMEM((joint, vocab), bf16),
            pltpu.VMEM((vocab // 128, 128), f32),
            pltpu.VMEM((n_utt, n_pos - 1), i32),
            pltpu.VMEM((n_utt, 128), i32),
            pltpu.SMEM((n_utt,), i32),
            pltpu.SMEM((n_utt,), i32),
            pltpu.VMEM((vocab, joint), bf16),
            pltpu.VMEM((vocab, 128), f32),
            pltpu.VMEM((n_slab, n_utt * t_local, 128), f32),
            pltpu.VMEM((n_slab, n_utt * n_pos, 128), f32),
            pltpu.VMEM((ITEMS * OCT, joint), bf16),
            pltpu.VMEM((2, vocab, 128), f32),
            pltpu.VMEM((t_local * n_pos, 128), f32),
            pltpu.VMEM((t_local * n_pos, 128), f32),
            pltpu.VMEM((128, 128), f32),
            pltpu.VMEM((2, tab_rows, 128), i32),
            pltpu.SMEM((2, tab_rows, 128), i32),
            pltpu.SemaphoreType.DMA((9,)),
            pltpu.SemaphoreType.DMA,
        ],
        name="joint",
    )(enc_blk.reshape(n_utt * t_local, d_enc), pred_out.reshape(n_utt * n_pos, d_pred), w_enc, w_pred, w_out,
      b_out.reshape(vocab // 128, 128), labels, frame_len, label_len)


def lattice_call(n_seq, matrices, label_len):
    n_hand, n_pos = matrices.shape[:2]
    n_utt = label_len.shape[0]
    f32 = jnp.float32
    return pl.pallas_call(
        functools.partial(lattice_kernel, n_seq),
        out_shape=jax.ShapeDtypeStruct((n_utt,), f32),
        in_specs=[pl.BlockSpec(memory_space=pl.ANY)] * 2,
        out_specs=pl.BlockSpec(memory_space=pltpu.VMEM),
        scratch_shapes=[
            pltpu.VMEM((n_seq, n_pos, 128), f32),
            pltpu.SMEM((n_utt,), jnp.int32),
            pltpu.VMEM((1, 128), f32),
            pltpu.VMEM((n_hand, 1, 128), f32),
            pltpu.SemaphoreType.DMA((n_hand,)),
            pltpu.SemaphoreType.DMA((n_seq,)),
            pltpu.SemaphoreType.DMA((n_seq,)),
            pltpu.SemaphoreType.DMA((n_hand,)),
            pltpu.SemaphoreType.DMA((2,)),
        ],
        compiler_params=pltpu.CompilerParams(collective_id=0, has_side_effects=True),
        name="lattice",
    )(matrices, label_len)


def solution(mesh):
    n_seq = mesh.shape["seq"]

    def local_loss(enc_blk, pred_out, w_enc, w_pred, w_out, b_out, labels, frame_len, label_len):
        matrices = joint_call(enc_blk, pred_out, w_enc, w_pred, w_out, b_out, labels, frame_len, label_len)
        return lattice_call(n_seq, matrices, label_len)

    in_specs = (P("dp", "seq", None), P("dp", None, None), P(), P(), P(), P(), P("dp", None), P("dp"), P("dp"))
    return jax.shard_map(local_loss, mesh=mesh, in_specs=in_specs, out_specs=P("dp"), check_vma=False)
```

```python
import functools
import jax
import jax.numpy as jnp
from jax import lax
from jax.experimental import pallas as pl
from jax.experimental.pallas import tpu as pltpu
from jax.sharding import PartitionSpec as P

NEG_FILL = -1.0e30
OCT = 8
ITEMS = 32
GROUP = 32
MESH = pl.DeviceIdType.MESH


def joint_kernel(enc_hbm, pred_hbm, wenc_hbm, wpred_hbm, wout_hbm, bout_hbm, lab_hbm, flen_hbm, llen_hbm,
                 m_out,
                 enc_v, pred_v, wenc_v, wpred_v, wout_v, bout_v, lab_raw, lab_v, flen_s, llen_s,
                 w_t, bias_t, a_v, c_v, hid, z_v, blank_d, label_d, turn_v, tab_v, tab_s, sems, tab_sem):
    n_utt, n_lab = lab_hbm.shape
    n_pos = n_lab + 1
    t_local = enc_v.shape[0] // n_utt
    n_oct = t_local // OCT
    joint, vocab = wout_v.shape
    n_slab = joint // 128
    rep = 128 // n_utt
    t0 = lax.axis_index("seq") * t_local

    copies = [
        pltpu.make_async_copy(src, dst, sems.at[k])
        for k, (src, dst) in enumerate([
            (flen_hbm, flen_s), (llen_hbm, llen_s), (lab_hbm, lab_raw), (bout_hbm, bout_v),
            (wout_hbm, wout_v), (enc_hbm, enc_v), (wenc_hbm, wenc_v), (pred_hbm, pred_v), (wpred_hbm, wpred_v)])
    ]
    for copy in copies:
        copy.start()

    blank_d[...] = jnp.zeros_like(blank_d)
    label_d[...] = jnp.full(label_d.shape, NEG_FILL, jnp.float32)

    for copy in copies[:3]:
        copy.wait()
    lab_v[...] = jnp.zeros_like(lab_v)
    lab_v[:, :n_lab] = lab_raw[...]
    shape = tab_v.shape[1:]
    cums, nus, total = [], [], jnp.int32(0)
    for b in range(n_utt):
        n_t = jnp.clip((flen_s[b] - t0 + OCT - 1) // OCT, 0, n_oct)
        cums.append(total)
        nus.append(llen_s[b] + 1)
        total = total + n_t * nus[b]
    lane = lax.broadcasted_iota(jnp.int32, shape, 1)
    item = lax.broadcasted_iota(jnp.int32, shape, 0) * ITEMS + lane % ITEMS
    item = jnp.minimum(item, total - 1)
    utt = jnp.zeros(shape, jnp.int32)
    base = jnp.zeros(shape, jnp.int32)
    width = jnp.ones(shape, jnp.int32)
    frames = jnp.zeros(shape, jnp.int32)
    for b in range(n_utt):
        hit = item >= cums[b]
        utt = jnp.where(hit, b, utt)
        base = jnp.where(hit, cums[b], base)
        width = jnp.where(hit, nus[b], width)
        frames = jnp.where(hit, flen_s[b] - t0, frames)
    rest = item - base
    octet = jnp.zeros(shape, jnp.int32)
    for k in range(1, n_oct):
        octet = octet + jnp.where(rest >= k * width, 1, 0)
    pos = jnp.clip(rest - octet * width, 0, n_pos - 1)
    word = jnp.zeros(shape, jnp.int32)
    for b in range(n_utt):
        row = jnp.broadcast_to(lab_v[b:b + 1, :], shape)
        word = jnp.where(utt == b, jnp.take_along_axis(row, pos, axis=1, mode="promise_in_bounds"), word)
    has_label = pos < width - 1
    word = jnp.where(has_label, word, 0)
    field = lane // ITEMS
    tab_v[0] = jnp.where(field == 0, utt * t_local + octet * OCT,
                         jnp.where(field == 1, utt * n_pos + pos,
                                   jnp.where(field == 2, word, (octet * n_pos + pos) * OCT)))
    tab_v[1] = jnp.where(field == 0, utt, jnp.where(field == 1, jnp.where(has_label, utt, -1), frames - octet * OCT))
    tab_copy = pltpu.make_async_copy(tab_v, tab_s, tab_sem)
    tab_copy.start()

    copies[3].wait()
    copies[4].wait()
    top_bias = jnp.max(bout_v[...])
    spread = jnp.zeros((8, 128), jnp.float32)
    for k in range(vocab // 128):
        cols = pl.ds(k * 128, 128)
        w_t[cols, :] = wout_v[:, cols].T
        bias_t[cols, :] = jnp.broadcast_to(bout_v[k:k + 1, :] - top_bias, (128, 128)).T
        mass = jnp.sum(jnp.abs(wout_v[:, cols].astype(jnp.float32)).reshape(joint // 8, 8, 128), axis=0)
        spread = jnp.maximum(spread, jnp.sum(mass, axis=0, keepdims=True))
    narrow = jnp.max(spread) <= 60.0
    copies[5].wait()
    copies[6].wait()
    proj = jnp.dot(enc_v[...], wenc_v[...], preferred_element_type=jnp.float32).astype(jnp.bfloat16).astype(jnp.float32)
    for s in range(n_slab):
        a_v[s] = proj[:, 128 * s:128 * s + 128]
    copies[7].wait()
    copies[8].wait()
    proj = jnp.dot(pred_v[...], wpred_v[...], preferred_element_type=jnp.float32).astype(jnp.bfloat16).astype(jnp.float32)
    for s in range(n_slab):
        c_v[s] = proj[:, 128 * s:128 * s + 128]
    tab_copy.wait()

    lane8 = lax.broadcasted_iota(jnp.int32, (OCT, 128), 1)
    frame8 = lax.broadcasted_iota(jnp.int32, (OCT, 128), 0)
    lane_utt = lane8 // rep
    lane_item = lax.broadcasted_iota(jnp.int32, (1, 128), 1) // OCT

    def make_hidden(tile):
        for q in range(ITEMS // 2):
            for s in range(n_slab):
                parts = []
                for k in (2 * q, 2 * q + 1):
                    a_row = pl.multiple_of(tab_s[0, tile, k], OCT)
                    parts.append(a_v[s, pl.ds(a_row, OCT), :] + c_v[s, pl.ds(tab_s[0, tile, ITEMS + k], 1), :])
                hid[16 * q:16 * q + 16, 128 * s:128 * s + 128] = jnp.tanh(
                    jnp.concatenate(parts, axis=0)).astype(jnp.bfloat16)

    def finish(tile, with_max):
        for g in range(2):
            label_z = jnp.zeros((1, 128), jnp.float32)
            for k in range(16):
                y = tab_s[0, tile, 2 * ITEMS + 16 * g + k]
                label_z = jnp.where(lane_item == k, z_v[g, pl.ds(y, 1), :] + bias_t[pl.ds(y, 1), :], label_z)
            blank_z = z_v[g, 0:1, :] + bias_t[0:1, :]
            top = jnp.zeros((1, 128), jnp.float32)
            if with_max:
                part = jnp.full((8, 128), NEG_FILL, jnp.float32)
                for k in range(vocab // 128):
                    rows = slice(k * 128, k * 128 + 128)
                    part = jnp.maximum(part, jnp.max((z_v[g, rows, :] + bias_t[rows, :]).reshape(16, 8, 128), axis=0))
                top = jnp.max(part, axis=0, keepdims=True)
            part = jnp.zeros((8, 128), jnp.float32)
            for k in range(vocab // 128):
                rows = slice(k * 128, k * 128 + 128)
                logit = z_v[g, rows, :] + bias_t[rows, :]
                if with_max:
                    logit = logit - top
                part = part + jnp.sum(jnp.exp(logit).reshape(16, 8, 128), axis=0)
            lse = jnp.log(jnp.sum(part, axis=0, keepdims=True)) + top
            blank_lp = jnp.broadcast_to(blank_z - lse, (OCT, 128))
            label_lp = jnp.broadcast_to(label_z - lse, (OCT, 128))
            for k in range(16):
                j = 16 * g + k
                live = frame8 < tab_s[1, tile, 2 * ITEMS + j]
                row = pl.ds(pl.multiple_of(tab_s[0, tile, 3 * ITEMS + j], OCT), OCT)
                pick = frame8 + OCT * k
                value = jnp.take_along_axis(blank_lp, pick, axis=1, mode="promise_in_bounds")
                pltpu.store(blank_d.at[row, :], value, mask=(lane_utt == tab_s[1, tile, j]) & live)
                value = jnp.take_along_axis(label_lp, pick, axis=1, mode="promise_in_bounds")
                pltpu.store(label_d.at[row, :], value, mask=(lane_utt == tab_s[1, tile, ITEMS + j]) & live)

    def matmul():
        z = lax.dot_general(w_t[...], hid[...], (((1,), (1,)), ((), ())), preferred_element_type=jnp.float32)
        z_v[0] = z[:, :128]
        z_v[1] = z[:, 128:]

    n_tiles = (total + ITEMS - 1) // ITEMS

    def run_tiles(with_max):
        make_hidden(0)
        matmul()
        make_hidden(jnp.minimum(1, n_tiles - 1))

        def step(i, _):
            finish(i - 1, with_max)
            matmul()
            make_hidden(jnp.minimum(i + 1, n_tiles - 1))
            return 0

        lax.fori_loop(1, n_tiles, step, 0)
        finish(n_tiles - 1, with_max)

    @pl.when((n_tiles > 0) & narrow)
    def _():
        run_tiles(False)

    @pl.when((n_tiles > 0) & jnp.logical_not(narrow))
    def _():
        run_tiles(True)

    entry = frame8 * rep + lane8 % rep
    stay = [jnp.where(entry == u, 0.0, NEG_FILL) for u in range(n_pos)]
    move = [None] * n_pos
    for d in range(t_local + n_pos - 1):
        for u in range(min(d, n_pos - 1), max(d - t_local, -1), -1):
            t = d - u
            row = (t // OCT * n_pos + u) * OCT + t % OCT
            if u == 0:
                alpha = stay[0]
            else:
                high, low = jnp.maximum(stay[u], move[u - 1]), jnp.minimum(stay[u], move[u - 1])
                alpha = high + jnp.log(1.0 + jnp.exp(low - high))
            stay[u] = alpha + blank_d[row:row + 1, :]
            move[u] = alpha + label_d[row:row + 1, :]
    for u in range(n_pos):
        for j in range(n_pos // rep):
            turn_v[GROUP * j + u:GROUP * j + u + 1, :] = stay[u][j:j + 1, :]
    turned = turn_v[...].T
    per = 128 // GROUP
    group = lane8 // GROUP
    for h in range(n_utt // per):
        for j in range(n_pos // rep):
            out = None
            for q in range(per):
                b = per * h + q
                piece = turned[rep * b:rep * b + rep, :]
                if q != j:
                    piece = pltpu.roll(piece, (GROUP * (q - j)) % 128, 1)
                out = piece if out is None else jnp.where(group == q, piece, out)
            m_out[h, rep * j:rep * j + rep, :] = out


def lattice_kernel(n_seq, m_hbm, llen_hbm, loss_ref,
                   m_recv, llen_s, v_out, v_recv, send_sem, recv_sem, out_sem, in_sem, own_sem):
    n_hand, n_pos = m_hbm.shape[:2]
    n_utt = llen_hbm.shape[0]
    per = 128 // GROUP
    me = lax.axis_index("seq")
    mine = me < n_hand
    my_hand = jnp.minimum(me, n_hand - 1)

    barrier = pltpu.get_barrier_semaphore()

    def greet(other):
        pl.semaphore_signal(barrier, inc=1, device_id={"seq": other}, device_id_type=MESH)

    @pl.when(mine)
    def _():
        for d in range(n_seq):
            @pl.when(me != d)
            def _():
                greet(d)

    own_len = pltpu.make_async_copy(llen_hbm, llen_s, own_sem.at[0])
    own_matrix = pltpu.make_async_copy(m_hbm.at[my_hand], m_recv.at[me], own_sem.at[1])

    @pl.when(mine)
    def _():
        own_len.start()
        own_matrix.start()

    pl.semaphore_wait(barrier, jnp.where(mine, n_hand - 1, n_hand))

    def send_matrix(h):
        return pltpu.make_async_remote_copy(
            src_ref=m_hbm.at[h], dst_ref=m_recv.at[me], send_sem=send_sem.at[h], recv_sem=recv_sem.at[me],
            device_id={"seq": h}, device_id_type=MESH)

    for h in range(n_hand):
        @pl.when(me != h)
        def _():
            send_matrix(h).start()

    def send_row(d):
        return pltpu.make_async_remote_copy(
            src_ref=v_out, dst_ref=v_recv.at[my_hand], send_sem=out_sem.at[d], recv_sem=in_sem.at[my_hand],
            device_id={"seq": d}, device_id_type=MESH)

    @pl.when(mine)
    def _():
        own_len.wait()
        own_matrix.wait()

        def arrived(src):
            @pl.when(src != me)
            def _():
                pltpu.make_async_remote_copy(
                    src_ref=m_hbm.at[0], dst_ref=m_recv.at[src], send_sem=send_sem.at[0], recv_sem=recv_sem.at[src],
                    device_id={"seq": src}, device_id_type=MESH).wait_recv()

        sub = lax.broadcasted_iota(jnp.int32, (n_pos, 128), 0)
        lane = lax.broadcasted_iota(jnp.int32, (n_pos, 128), 1)
        turn_idx = lane // GROUP * GROUP + sub

        def join(src, row):
            arrived(src)
            col = jnp.take_along_axis(jnp.broadcast_to(row, (n_pos, 128)), turn_idx, axis=1, mode="promise_in_bounds")
            terms = col + m_recv[src]
            top = jnp.max(terms, axis=0, keepdims=True)
            return top + jnp.log(jnp.sum(jnp.exp(terms - top), axis=0, keepdims=True))

        arrived(jnp.int32(0))
        row = m_recv[0, 0:1, :]
        row = lax.fori_loop(1, n_seq, join, row)
        sub8 = lax.broadcasted_iota(jnp.int32, (8, 128), 0)
        lane8 = lax.broadcasted_iota(jnp.int32, (8, 128), 1)
        want = jnp.full((8, 128), -1, jnp.int32)
        for b in range(n_utt):
            want = jnp.where(my_hand * per + sub8 == b, llen_s[b], want)
        keep = (lane8 // GROUP == sub8) & (lane8 % GROUP == want)
        column = jnp.sum(jnp.where(keep, row, 0.0), axis=1, keepdims=True)
        here = (lane8 == my_hand * per + sub8) & (sub8 < per)
        v_out[...] = jnp.sum(jnp.where(here, column, 0.0), axis=0, keepdims=True)
        for d in range(n_seq):
            @pl.when(me != d)
            def _():
                send_row(d).start()
        v_recv[my_hand] = v_out[...]

    for h in range(n_hand):
        @pl.when(me != h)
        def _():
            pltpu.make_async_remote_copy(
                src_ref=v_out, dst_ref=v_recv.at[h], send_sem=out_sem.at[0], recv_sem=in_sem.at[h],
                device_id={"seq": h}, device_id_type=MESH).wait_recv()
    total = v_recv[0]
    for h in range(1, n_hand):
        total = total + v_recv[h]
    loss_ref[...] = -total[0, :n_utt]

    for h in range(n_hand):
        @pl.when(me != h)
        def _():
            send_matrix(h).wait_send()

    @pl.when(mine)
    def _():
        for d in range(n_seq):
            @pl.when(me != d)
            def _():
                send_row(d).wait_send()


def joint_call(enc_blk, pred_out, w_enc, w_pred, w_out, b_out, labels, frame_len, label_len):
    n_utt, t_local, d_enc = enc_blk.shape
    n_pos, d_pred = pred_out.shape[1:]
    joint, vocab = w_out.shape
    n_oct = t_local // OCT
    n_slab = joint // 128
    per = 128 // GROUP
    tab_rows = -(-(n_utt * n_pos * n_oct // ITEMS + 1) // 8) * 8
    hbm = pl.BlockSpec(memory_space=pl.ANY)
    vmem = pl.BlockSpec(memory_space=pltpu.VMEM)
    f32, bf16, i32 = jnp.float32, jnp.bfloat16, jnp.int32
    return pl.pallas_call(
        joint_kernel,
        out_shape=pltpu.VMEM((n_utt // per, n_pos, 128), f32),
        in_specs=[hbm] * 9,
        out_specs=vmem,
        scratch_shapes=[
            pltpu.VMEM((n_utt * t_local, d_enc), bf16),
            pltpu.VMEM((n_utt * n_pos, d_pred), bf16),
            pltpu.VMEM((d_enc, joint), bf16),
            pltpu.VMEM((d_pred, joint), bf16),
            pltpu.VMEM((joint, vocab), bf16),
            pltpu.VMEM((vocab // 128, 128), f32),
            pltpu.VMEM((n_utt, n_pos - 1), i32),
            pltpu.VMEM((n_utt, 128), i32),
            pltpu.SMEM((n_utt,), i32),
            pltpu.SMEM((n_utt,), i32),
            pltpu.VMEM((vocab, joint), bf16),
            pltpu.VMEM((vocab, 128), f32),
            pltpu.VMEM((n_slab, n_utt * t_local, 128), f32),
            pltpu.VMEM((n_slab, n_utt * n_pos, 128), f32),
            pltpu.VMEM((ITEMS * OCT, joint), bf16),
            pltpu.VMEM((2, vocab, 128), f32),
            pltpu.VMEM((t_local * n_pos, 128), f32),
            pltpu.VMEM((t_local * n_pos, 128), f32),
            pltpu.VMEM((128, 128), f32),
            pltpu.VMEM((2, tab_rows, 128), i32),
            pltpu.SMEM((2, tab_rows, 128), i32),
            pltpu.SemaphoreType.DMA((9,)),
            pltpu.SemaphoreType.DMA,
        ],
        name="joint",
    )(enc_blk.reshape(n_utt * t_local, d_enc), pred_out.reshape(n_utt * n_pos, d_pred), w_enc, w_pred, w_out,
      b_out.reshape(vocab // 128, 128), labels, frame_len, label_len)


def lattice_call(n_seq, matrices, label_len):
    n_hand, n_pos = matrices.shape[:2]
    n_utt = label_len.shape[0]
    f32 = jnp.float32
    return pl.pallas_call(
        functools.partial(lattice_kernel, n_seq),
        out_shape=pltpu.VMEM((n_utt,), f32),
        in_specs=[pl.BlockSpec(memory_space=pltpu.VMEM), pl.BlockSpec(memory_space=pl.ANY)],
        out_specs=pl.BlockSpec(memory_space=pltpu.VMEM),
        scratch_shapes=[
            pltpu.VMEM((n_seq, n_pos, 128), f32),
            pltpu.SMEM((n_utt,), jnp.int32),
            pltpu.VMEM((1, 128), f32),
            pltpu.VMEM((n_hand, 1, 128), f32),
            pltpu.SemaphoreType.DMA((n_hand,)),
            pltpu.SemaphoreType.DMA((n_seq,)),
            pltpu.SemaphoreType.DMA((n_seq,)),
            pltpu.SemaphoreType.DMA((n_hand,)),
            pltpu.SemaphoreType.DMA((2,)),
        ],
        compiler_params=pltpu.CompilerParams(collective_id=0, has_side_effects=True),
        name="lattice",
    )(matrices, label_len)


def solution(mesh):
    n_seq = mesh.shape["seq"]

    def local_loss(enc_blk, pred_out, w_enc, w_pred, w_out, b_out, labels, frame_len, label_len):
        matrices = joint_call(enc_blk, pred_out, w_enc, w_pred, w_out, b_out, labels, frame_len, label_len)
        return lattice_call(n_seq, pltpu.with_memory_space_constraint(matrices, pltpu.VMEM), label_len)

    in_specs = (P("dp", "seq", None), P("dp", None, None), P(), P(), P(), P(), P("dp", None), P("dp"), P("dp"))
    return jax.shard_map(local_loss, mesh=mesh, in_specs=in_specs, out_specs=P("dp"), check_vma=False)
```

```python
import functools
import jax
import jax.numpy as jnp
from jax import lax
from jax.experimental import pallas as pl
from jax.experimental.pallas import tpu as pltpu
from jax.sharding import PartitionSpec as P

NEG_FILL = -1.0e30
OCT = 8
ITEMS = 32
GROUP = 32
MESH = pl.DeviceIdType.MESH


def joint_kernel(enc_hbm, pred_hbm, wenc_hbm, wpred_hbm, wout_hbm, bout_hbm, lab_hbm, flen_hbm, llen_hbm,
                 m_out,
                 enc_v, pred_v, wenc_v, wpred_v, wout_v, bout_v, lab_raw, lab_v, flen_s, llen_s,
                 w_t, bias_t, a_v, c_v, hid, z_v, lp_v, both_d, blank_d, label_d, turn_v, tab_v, tab_s, sems, tab_sem):
    n_utt, n_lab = lab_hbm.shape
    n_pos = n_lab + 1
    t_local = enc_v.shape[0] // n_utt
    n_oct = t_local // OCT
    joint, vocab = wout_v.shape
    n_slab = joint // 128
    half = 64
    rep = half // n_utt
    t0 = lax.axis_index("seq") * t_local

    copies = [
        pltpu.make_async_copy(src, dst, sems.at[k])
        for k, (src, dst) in enumerate([
            (flen_hbm, flen_s), (llen_hbm, llen_s), (lab_hbm, lab_raw), (bout_hbm, bout_v),
            (wout_hbm, wout_v), (enc_hbm, enc_v), (wenc_hbm, wenc_v), (pred_hbm, pred_v), (wpred_hbm, wpred_v)])
    ]
    for copy in copies:
        copy.start()

    both_d[...] = jnp.where(lax.broadcasted_iota(jnp.int32, both_d.shape, 1) < half, 0.0, NEG_FILL)

    for copy in copies[:3]:
        copy.wait()
    lab_v[...] = jnp.zeros_like(lab_v)
    lab_v[:, :n_lab] = lab_raw[...]
    shape = tab_v.shape[1:]
    cums, nus, total = [], [], jnp.int32(0)
    for b in range(n_utt):
        n_t = jnp.clip((flen_s[b] - t0 + OCT - 1) // OCT, 0, n_oct)
        cums.append(total)
        nus.append(llen_s[b] + 1)
        total = total + n_t * nus[b]
    lane = lax.broadcasted_iota(jnp.int32, shape, 1)
    item = lax.broadcasted_iota(jnp.int32, shape, 0) * ITEMS + lane % ITEMS
    item = jnp.minimum(item, total - 1)
    utt = jnp.zeros(shape, jnp.int32)
    base = jnp.zeros(shape, jnp.int32)
    width = jnp.ones(shape, jnp.int32)
    for b in range(n_utt):
        hit = item >= cums[b]
        utt = jnp.where(hit, b, utt)
        base = jnp.where(hit, cums[b], base)
        width = jnp.where(hit, nus[b], width)
    rest = item - base
    octet = jnp.zeros(shape, jnp.int32)
    for k in range(1, n_oct):
        octet = octet + jnp.where(rest >= k * width, 1, 0)
    pos = jnp.clip(rest - octet * width, 0, n_pos - 1)
    word = jnp.zeros(shape, jnp.int32)
    for b in range(n_utt):
        row = jnp.broadcast_to(lab_v[b:b + 1, :], shape)
        word = jnp.where(utt == b, jnp.take_along_axis(row, pos, axis=1, mode="promise_in_bounds"), word)
    word = jnp.where(pos < width - 1, word, vocab)
    field = lane // ITEMS
    tab_v[0] = jnp.where(field == 0, utt * t_local + octet * OCT,
                         jnp.where(field == 1, utt * n_pos + pos,
                                   jnp.where(field == 2, word, (octet * n_pos + pos) * OCT)))
    tab_v[1] = utt
    tab_copy = pltpu.make_async_copy(tab_v, tab_s, tab_sem)
    tab_copy.start()

    copies[3].wait()
    copies[4].wait()
    top_bias = jnp.max(bout_v[...])
    bias_t[vocab:, :] = jnp.full((8, 128), NEG_FILL, jnp.float32)
    z_v[:, :, vocab:, :] = jnp.zeros((2, 2, 8, 128), jnp.float32)
    spread = jnp.zeros((8, 128), jnp.float32)
    for k in range(vocab // 128):
        cols = pl.ds(k * 128, 128)
        w_t[cols, :] = wout_v[:, cols].T
        bias_t[cols, :] = jnp.broadcast_to(bout_v[k:k + 1, :] - top_bias, (128, 128)).T
        mass = jnp.sum(jnp.abs(wout_v[:, cols].astype(jnp.float32)).reshape(joint // 8, 8, 128), axis=0)
        spread = jnp.maximum(spread, jnp.sum(mass, axis=0, keepdims=True))
    narrow = jnp.max(spread) <= 60.0
    copies[5].wait()
    copies[6].wait()
    proj = jnp.dot(enc_v[...], wenc_v[...], preferred_element_type=jnp.float32).astype(jnp.bfloat16).astype(jnp.float32)
    for s in range(n_slab):
        a_v[s] = proj[:, 128 * s:128 * s + 128]
    copies[7].wait()
    copies[8].wait()
    proj = jnp.dot(pred_v[...], wpred_v[...], preferred_element_type=jnp.float32).astype(jnp.bfloat16).astype(jnp.float32)
    for s in range(n_slab):
        c_v[s] = proj[:, 128 * s:128 * s + 128]
    tab_copy.wait()

    lane8 = lax.broadcasted_iota(jnp.int32, (OCT, 128), 1)
    frame8 = lax.broadcasted_iota(jnp.int32, (OCT, 128), 0)
    lane_utt = lane8 % half // rep
    lane_item = lax.broadcasted_iota(jnp.int32, (1, 128), 1) // OCT

    def make_hidden(tile, slot):
        for q in range(ITEMS // 2):
            pair = (2 * q, 2 * q + 1)
            a_rows = [pl.ds(pl.multiple_of(tab_s[0, tile, k], OCT), OCT) for k in pair]
            c_rows = [pl.ds(tab_s[0, tile, ITEMS + k], 1) for k in pair]
            for s in range(n_slab):
                total_in = [a_v[s, a_row, :] + c_v[s, c_row, :] for a_row, c_row in zip(a_rows, c_rows)]
                hid[slot, 16 * q:16 * q + 16, 128 * s:128 * s + 128] = jnp.tanh(
                    jnp.concatenate(total_in, axis=0)).astype(jnp.bfloat16)

    def finish(tile, slot, with_max):
        for g in range(2):
            label_z = jnp.zeros((1, 128), jnp.float32)
            for k in range(16):
                y = pl.ds(tab_s[0, tile, 2 * ITEMS + 16 * g + k], 1)
                label_z = jnp.where(lane_item == k, z_v[slot, g, y, :] + bias_t[y, :], label_z)
            blank_z = z_v[slot, g, 0:1, :] + bias_t[0:1, :]
            top = jnp.zeros((1, 128), jnp.float32)
            if with_max:
                part = jnp.full((8, 128), NEG_FILL, jnp.float32)
                for k in range(vocab // 128):
                    rows = slice(k * 128, k * 128 + 128)
                    part = jnp.maximum(
                        part, jnp.max((z_v[slot, g, rows, :] + bias_t[rows, :]).reshape(16, 8, 128), axis=0))
                top = jnp.max(part, axis=0, keepdims=True)
            part = jnp.zeros((8, 128), jnp.float32)
            for k in range(vocab // 128):
                rows = slice(k * 128, k * 128 + 128)
                logit = z_v[slot, g, rows, :] + bias_t[rows, :]
                if with_max:
                    logit = logit - top
                part = part + jnp.sum(jnp.exp(logit).reshape(16, 8, 128), axis=0)
            lse = jnp.log(jnp.sum(part, axis=0, keepdims=True)) + top
            lp_v[slot, g, 0:1, :] = blank_z - lse
            lp_v[slot, g, 1:2, :] = label_z - lse

    def place(tile, slot):
        for g in range(2):
            wide = jnp.concatenate([jnp.broadcast_to(lp_v[slot, g, 0:1, :], (half, 128)),
                                    jnp.broadcast_to(lp_v[slot, g, 1:2, :], (half, 128))], axis=0).T
            for k in range(16):
                row = pl.ds(pl.multiple_of(tab_s[0, tile, 3 * ITEMS + 16 * g + k], OCT), OCT)
                pltpu.store(both_d.at[row, :], wide[OCT * k:OCT * k + OCT, :],
                            mask=lane_utt == tab_s[1, tile, 16 * g + k])

    def matmul(slot):
        z = lax.dot_general(w_t[...], hid[slot], (((1,), (1,)), ((), ())), preferred_element_type=jnp.float32)
        for g in range(2):
            z_v[slot, g, :vocab, :] = z[:, 128 * g:128 * g + 128]

    n_tiles = (total + ITEMS - 1) // ITEMS

    @pl.when((n_tiles > 0) & narrow)
    def _():
        make_hidden(0, 0)
        matmul(0)
        make_hidden(1, 1)

        def two_tiles(p, _):
            i = 2 * p + 1
            place(jnp.maximum(i - 2, 1), 1)
            place(jnp.maximum(i - 3, 0), 0)
            finish(i - 1, 0, False)
            matmul(1)
            make_hidden(i + 1, 0)
            finish(i, 1, False)
            matmul(0)
            make_hidden(i + 2, 1)
            return 0

        n_pairs = (n_tiles - 1) // 2
        lax.fori_loop(0, n_pairs, two_tiles, 0)
        place(jnp.maximum(2 * n_pairs - 1, 1), 1)
        place(jnp.maximum(2 * n_pairs - 2, 0), 0)
        finish(2 * n_pairs, 0, False)

        @pl.when(n_tiles % 2 == 0)
        def _():
            matmul(1)
            finish(n_tiles - 1, 1, False)

        place(2 * n_pairs + 1, 1)
        place(2 * n_pairs, 0)

    @pl.when((n_tiles > 0) & jnp.logical_not(narrow))
    def _():
        def one_tile(i, _):
            make_hidden(i, 0)
            matmul(0)
            finish(i, 0, True)
            place(i, 0)
            return 0

        lax.fori_loop(0, n_tiles, one_tile, 0)

    flen = jnp.zeros((OCT, 128), jnp.int32)
    for b in range(n_utt):
        flen = jnp.where(lane_utt == b, flen_s[b] - t0, flen)
    for k in range(n_oct):
        live = k * OCT + frame8 < flen
        for u in range(n_pos):
            rows = slice((k * n_pos + u) * OCT, (k * n_pos + u + 1) * OCT)
            both = both_d[rows, :]
            blank_d[rows, :] = jnp.where(live, both, 0.0)
            label_d[rows, :] = jnp.where(live, pltpu.roll(both, half, 1), NEG_FILL)

    entry = frame8 * rep + lane8 % rep
    stay = [jnp.where(entry == u, 0.0, NEG_FILL) for u in range(n_pos)]
    move = [None] * n_pos
    for d in range(t_local + n_pos - 1):
        for u in range(min(d, n_pos - 1), max(d - t_local, -1), -1):
            t = d - u
            row = (t // OCT * n_pos + u) * OCT + t % OCT
            if u == 0:
                alpha = stay[0]
            else:
                high, low = jnp.maximum(stay[u], move[u - 1]), jnp.minimum(stay[u], move[u - 1])
                alpha = high + jnp.log(1.0 + jnp.exp(low - high))
            stay[u] = alpha + blank_d[row:row + 1, :]
            move[u] = alpha + label_d[row:row + 1, :]
    n_turn = n_pos // rep
    for u in range(n_pos):
        for j in range(n_turn):
            turn_v[j // 4, GROUP * (j % 4) + u:GROUP * (j % 4) + u + 1, :] = stay[u][j:j + 1, :]
    per = 128 // GROUP
    group = lane8 // GROUP
    lower = frame8 < rep
    turned = [turn_v[k].T[:half, :] for k in range(2)]
    shifted = {}
    for h in range(n_utt // per):
        for i in range(n_turn // 2):
            out = None
            for q in range(per):
                vreg = (per * h + q) // 2
                pieces = []
                for c in range(2):
                    j = 2 * i + c
                    key = (j // 4, vreg, (q - j) % 4, (q % 2) != c)
                    if key not in shifted:
                        piece = turned[key[0]][8 * vreg:8 * vreg + 8, :]
                        if key[2]:
                            piece = pltpu.roll(piece, GROUP * key[2], 1)
                        if key[3]:
                            piece = pltpu.roll(piece, rep, 0)
                        shifted[key] = piece
                    pieces.append(shifted[key])
                piece = jnp.where(lower, pieces[0], pieces[1])
                out = piece if out is None else jnp.where(group == q, piece, out)
            m_out[h, 8 * i:8 * i + 8, :] = out


def lattice_kernel(n_seq, m_hbm, llen_hbm, loss_ref,
                   m_recv, llen_s, v_out, v_recv, send_sem, recv_sem, out_sem, in_sem, own_sem):
    n_hand, n_pos = m_hbm.shape[:2]
    n_utt = llen_hbm.shape[0]
    per = 128 // GROUP
    me = lax.axis_index("seq")
    mine = me < n_hand
    my_hand = jnp.minimum(me, n_hand - 1)

    barrier = pltpu.get_barrier_semaphore()

    def greet(other):
        pl.semaphore_signal(barrier, inc=1, device_id={"seq": other}, device_id_type=MESH)

    @pl.when(mine)
    def _():
        for d in range(n_seq):
            @pl.when(me != d)
            def _():
                greet(d)

    own_len = pltpu.make_async_copy(llen_hbm, llen_s, own_sem.at[0])
    own_matrix = pltpu.make_async_copy(m_hbm.at[my_hand], m_recv.at[me], own_sem.at[1])

    @pl.when(mine)
    def _():
        own_len.start()
        own_matrix.start()

    pl.semaphore_wait(barrier, jnp.where(mine, n_hand - 1, n_hand))

    def send_matrix(h):
        return pltpu.make_async_remote_copy(
            src_ref=m_hbm.at[h], dst_ref=m_recv.at[me], send_sem=send_sem.at[h], recv_sem=recv_sem.at[me],
            device_id={"seq": h}, device_id_type=MESH)

    for h in range(n_hand):
        @pl.when(me != h)
        def _():
            send_matrix(h).start()

    def send_row(d):
        return pltpu.make_async_remote_copy(
            src_ref=v_out, dst_ref=v_recv.at[my_hand], send_sem=out_sem.at[d], recv_sem=in_sem.at[my_hand],
            device_id={"seq": d}, device_id_type=MESH)

    @pl.when(mine)
    def _():
        own_len.wait()
        own_matrix.wait()

        def arrived(src):
            @pl.when(src != me)
            def _():
                pltpu.make_async_remote_copy(
                    src_ref=m_hbm.at[0], dst_ref=m_recv.at[src], send_sem=send_sem.at[0], recv_sem=recv_sem.at[src],
                    device_id={"seq": src}, device_id_type=MESH).wait_recv()

        sub = lax.broadcasted_iota(jnp.int32, (n_pos, 128), 0)
        lane = lax.broadcasted_iota(jnp.int32, (n_pos, 128), 1)
        turn_idx = lane // GROUP * GROUP + sub

        def join(src, row):
            arrived(src)
            col = jnp.take_along_axis(jnp.broadcast_to(row, (n_pos, 128)), turn_idx, axis=1, mode="promise_in_bounds")
            terms = col + m_recv[src]
            top = jnp.max(terms, axis=0, keepdims=True)
            return top + jnp.log(jnp.sum(jnp.exp(terms - top), axis=0, keepdims=True))

        arrived(jnp.int32(0))
        row = m_recv[0, 0:1, :]
        row = lax.fori_loop(1, n_seq, join, row)
        sub8 = lax.broadcasted_iota(jnp.int32, (8, 128), 0)
        lane8 = lax.broadcasted_iota(jnp.int32, (8, 128), 1)
        want = jnp.full((8, 128), -1, jnp.int32)
        for b in range(n_utt):
            want = jnp.where(my_hand * per + sub8 == b, llen_s[b], want)
        keep = (lane8 // GROUP == sub8) & (lane8 % GROUP == want)
        column = jnp.sum(jnp.where(keep, row, 0.0), axis=1, keepdims=True)
        here = (lane8 == my_hand * per + sub8) & (sub8 < per)
        v_out[...] = jnp.sum(jnp.where(here, column, 0.0), axis=0, keepdims=True)
        for d in range(n_seq):
            @pl.when(me != d)
            def _():
                send_row(d).start()
        v_recv[my_hand] = v_out[...]

    for h in range(n_hand):
        @pl.when(me != h)
        def _():
            pltpu.make_async_remote_copy(
                src_ref=v_out, dst_ref=v_recv.at[h], send_sem=out_sem.at[0], recv_sem=in_sem.at[h],
                device_id={"seq": h}, device_id_type=MESH).wait_recv()
    total = v_recv[0]
    for h in range(1, n_hand):
        total = total + v_recv[h]
    loss_ref[...] = -total[0, :n_utt]

    for h in range(n_hand):
        @pl.when(me != h)
        def _():
            send_matrix(h).wait_send()

    @pl.when(mine)
    def _():
        for d in range(n_seq):
            @pl.when(me != d)
            def _():
                send_row(d).wait_send()


def joint_call(enc_blk, pred_out, w_enc, w_pred, w_out, b_out, labels, frame_len, label_len):
    n_utt, t_local, d_enc = enc_blk.shape
    n_pos, d_pred = pred_out.shape[1:]
    joint, vocab = w_out.shape
    n_oct = t_local // OCT
    n_slab = joint // 128
    per = 128 // GROUP
    tab_rows = -(-(n_utt * n_pos * n_oct // ITEMS + 2) // 8) * 8
    hbm = pl.BlockSpec(memory_space=pl.ANY)
    vmem = pl.BlockSpec(memory_space=pltpu.VMEM)
    f32, bf16, i32 = jnp.float32, jnp.bfloat16, jnp.int32
    return pl.pallas_call(
        joint_kernel,
        out_shape=pltpu.VMEM((n_utt // per, n_pos, 128), f32),
        in_specs=[hbm] * 9,
        out_specs=vmem,
        scratch_shapes=[
            pltpu.VMEM((n_utt * t_local, d_enc), bf16),
            pltpu.VMEM((n_utt * n_pos, d_pred), bf16),
            pltpu.VMEM((d_enc, joint), bf16),
            pltpu.VMEM((d_pred, joint), bf16),
            pltpu.VMEM((joint, vocab), bf16),
            pltpu.VMEM((vocab // 128, 128), f32),
            pltpu.VMEM((n_utt, n_pos - 1), i32),
            pltpu.VMEM((n_utt, 128), i32),
            pltpu.SMEM((n_utt,), i32),
            pltpu.SMEM((n_utt,), i32),
            pltpu.VMEM((vocab, joint), bf16),
            pltpu.VMEM((vocab + 8, 128), f32),
            pltpu.VMEM((n_slab, n_utt * t_local, 128), f32),
            pltpu.VMEM((n_slab, n_utt * n_pos, 128), f32),
            pltpu.VMEM((2, ITEMS * OCT, joint), bf16),
            pltpu.VMEM((2, 2, vocab + 8, 128), f32),
            pltpu.VMEM((2, 2, 8, 128), f32),
            pltpu.VMEM((t_local * n_pos, 128), f32),
            pltpu.VMEM((t_local * n_pos, 128), f32),
            pltpu.VMEM((t_local * n_pos, 128), f32),
            pltpu.VMEM((2, 128, 128), f32),
            pltpu.VMEM((2, tab_rows, 128), i32),
            pltpu.SMEM((2, tab_rows, 128), i32),
            pltpu.SemaphoreType.DMA((9,)),
            pltpu.SemaphoreType.DMA,
        ],
        name="joint",
    )(enc_blk.reshape(n_utt * t_local, d_enc), pred_out.reshape(n_utt * n_pos, d_pred), w_enc, w_pred, w_out,
      b_out.reshape(vocab // 128, 128), labels, frame_len, label_len)


def lattice_call(n_seq, matrices, label_len):
    n_hand, n_pos = matrices.shape[:2]
    n_utt = label_len.shape[0]
    f32 = jnp.float32
    return pl.pallas_call(
        functools.partial(lattice_kernel, n_seq),
        out_shape=pltpu.VMEM((n_utt,), f32),
        in_specs=[pl.BlockSpec(memory_space=pltpu.VMEM), pl.BlockSpec(memory_space=pl.ANY)],
        out_specs=pl.BlockSpec(memory_space=pltpu.VMEM),
        scratch_shapes=[
            pltpu.VMEM((n_seq, n_pos, 128), f32),
            pltpu.SMEM((n_utt,), jnp.int32),
            pltpu.VMEM((1, 128), f32),
            pltpu.VMEM((n_hand, 1, 128), f32),
            pltpu.SemaphoreType.DMA((n_hand,)),
            pltpu.SemaphoreType.DMA((n_seq,)),
            pltpu.SemaphoreType.DMA((n_seq,)),
            pltpu.SemaphoreType.DMA((n_hand,)),
            pltpu.SemaphoreType.DMA((2,)),
        ],
        compiler_params=pltpu.CompilerParams(collective_id=0, has_side_effects=True),
        name="lattice",
    )(matrices, label_len)


def solution(mesh):
    n_seq = mesh.shape["seq"]

    def local_loss(enc_blk, pred_out, w_enc, w_pred, w_out, b_out, labels, frame_len, label_len):
        matrices = joint_call(enc_blk, pred_out, w_enc, w_pred, w_out, b_out, labels, frame_len, label_len)
        return lattice_call(n_seq, pltpu.with_memory_space_constraint(matrices, pltpu.VMEM), label_len)

    in_specs = (P("dp", "seq", None), P("dp", None, None), P(), P(), P(), P(), P("dp", None), P("dp"), P("dp"))
    return jax.shard_map(local_loss, mesh=mesh, in_specs=in_specs, out_specs=P("dp"), check_vma=False)
```

```python
import functools
import jax
import jax.numpy as jnp
from jax import lax
from jax.experimental import pallas as pl
from jax.experimental.pallas import tpu as pltpu
from jax.sharding import PartitionSpec as P

NEG_FILL = -1.0e30
OCT = 8
TILE = 256
FIELD = 16
GROUP = 32
MESH = pl.DeviceIdType.MESH


def joint_kernel(enc_hbm, pred_hbm, wenc_hbm, wpred_hbm, wout_hbm, bout_hbm, lab_hbm, flen_hbm, llen_hbm,
                 m_out,
                 enc_v, pred_v, wenc_v, wpred_v, wout_v, bout_v, lab_raw, lab_v, flen_s, llen_s,
                 w_t, bias_t, a_v, c_v, hid, z_v, lp_v, both_d, blank_d, label_d, turn_v, tab_v, tab_s, sems, tab_sem):
    n_utt, n_lab = lab_hbm.shape
    n_pos = n_lab + 1
    t_local = enc_v.shape[0] // n_utt
    n_oct = t_local // OCT
    items = TILE // t_local
    joint, vocab = wout_v.shape
    n_slab = joint // 128
    half = 64
    rep = half // n_utt
    t0 = lax.axis_index("seq") * t_local

    copies = [
        pltpu.make_async_copy(src, dst, sems.at[k])
        for k, (src, dst) in enumerate([
            (flen_hbm, flen_s), (llen_hbm, llen_s), (lab_hbm, lab_raw), (bout_hbm, bout_v),
            (wout_hbm, wout_v), (enc_hbm, enc_v), (wenc_hbm, wenc_v), (pred_hbm, pred_v), (wpred_hbm, wpred_v)])
    ]
    for copy in copies:
        copy.start()

    both_d[...] = jnp.where(lax.broadcasted_iota(jnp.int32, both_d.shape, 1) < half, 0.0, NEG_FILL)

    for copy in copies[:3]:
        copy.wait()
    lab_v[...] = jnp.zeros_like(lab_v)
    lab_v[:, :n_lab] = lab_raw[...]
    shape = tab_v.shape
    cums, nus, total = [], [], jnp.int32(0)
    for b in range(n_utt):
        cums.append(total)
        nus.append(llen_s[b] + 1)
        total = total + jnp.where(flen_s[b] > t0, nus[b], 0)
    lane = lax.broadcasted_iota(jnp.int32, shape, 1)
    item = lax.broadcasted_iota(jnp.int32, shape, 0) * items + jnp.minimum(lane % FIELD, items - 1)
    item = jnp.minimum(item, total - 1)
    utt = jnp.zeros(shape, jnp.int32)
    base = jnp.zeros(shape, jnp.int32)
    width = jnp.ones(shape, jnp.int32)
    for b in range(n_utt):
        hit = item >= cums[b]
        utt = jnp.where(hit, b, utt)
        base = jnp.where(hit, cums[b], base)
        width = jnp.where(hit, nus[b], width)
    pos = jnp.clip(item - base, 0, n_pos - 1)
    word = jnp.zeros(shape, jnp.int32)
    for b in range(n_utt):
        row = jnp.broadcast_to(lab_v[b:b + 1, :], shape)
        word = jnp.where(utt == b, jnp.take_along_axis(row, pos, axis=1, mode="promise_in_bounds"), word)
    word = jnp.where(pos < width - 1, word, vocab)
    field = lane // FIELD
    tab_v[...] = jnp.where(field == 0, utt * t_local,
                           jnp.where(field == 1, utt * n_pos + pos,
                                     jnp.where(field == 2, word, jnp.where(field == 3, pos * t_local, utt))))
    tab_copy = pltpu.make_async_copy(tab_v, tab_s, tab_sem)
    tab_copy.start()

    copies[3].wait()
    copies[4].wait()
    top_bias = jnp.max(bout_v[...])
    bias_t[vocab:, :] = jnp.full((8, 128), NEG_FILL, jnp.float32)
    z_v[:, :, vocab:, :] = jnp.zeros((2, 2, 8, 128), jnp.float32)
    spread = jnp.zeros((8, 128), jnp.float32)
    for k in range(vocab // 128):
        cols = pl.ds(k * 128, 128)
        w_t[cols, :] = wout_v[:, cols].T
        bias_t[cols, :] = jnp.broadcast_to(bout_v[k:k + 1, :] - top_bias, (128, 128)).T
        mass = jnp.sum(jnp.abs(wout_v[:, cols].astype(jnp.float32)).reshape(joint // 8, 8, 128), axis=0)
        spread = jnp.maximum(spread, jnp.sum(mass, axis=0, keepdims=True))
    narrow = jnp.max(spread) <= 60.0
    copies[5].wait()
    copies[6].wait()
    proj = jnp.dot(enc_v[...], wenc_v[...], preferred_element_type=jnp.float32).astype(jnp.bfloat16).astype(jnp.float32)
    for s in range(n_slab):
        a_v[s] = proj[:, 128 * s:128 * s + 128]
    copies[7].wait()
    copies[8].wait()
    proj = jnp.dot(pred_v[...], wpred_v[...], preferred_element_type=jnp.float32).astype(jnp.bfloat16).astype(jnp.float32)
    for s in range(n_slab):
        c_v[s] = proj[:, 128 * s:128 * s + 128]
    tab_copy.wait()

    lane8 = lax.broadcasted_iota(jnp.int32, (OCT, 128), 1)
    frame8 = lax.broadcasted_iota(jnp.int32, (OCT, 128), 0)
    lane_utt = lane8 % half // rep
    lane_item = [(lax.broadcasted_iota(jnp.int32, (1, 128), 1) + 128 * g) // t_local for g in range(2)]
    n_chunk = 4
    rows_chunk = vocab // n_chunk

    def entry_of(tile, which, k):
        return tab_s[tile, FIELD * which + k]

    def hidden_chunk(tile, slot, c):
        for q in range(items // 2):
            if q * n_chunk // (items // 2) != c:
                continue
            pair = (2 * q, 2 * q + 1)
            a_rows = [pl.ds(pl.multiple_of(entry_of(tile, 0, k), OCT), t_local) for k in pair]
            c_rows = [pl.ds(entry_of(tile, 1, k), 1) for k in pair]
            rows = slice(2 * t_local * q, 2 * t_local * (q + 1))
            for s in range(n_slab):
                total_in = [a_v[s, a_row, :] + c_v[s, c_row, :] for a_row, c_row in zip(a_rows, c_rows)]
                hid[slot, rows, 128 * s:128 * s + 128] = jnp.tanh(
                    jnp.concatenate(total_in, axis=0)).astype(jnp.bfloat16)

    def logits(slot, g, rows):
        return z_v[slot, g, rows, :] + bias_t[rows, :]

    def label_row(tile, slot, g):
        value = jnp.zeros((1, 128), jnp.float32)
        for k in range(128 * g // t_local, min(items, (128 * g + 127) // t_local + 1)):
            value = jnp.where(lane_item[g] == k, logits(slot, g, pl.ds(entry_of(tile, 2, k), 1)), value)
        return value

    def sum_chunk(slot, c, parts, tops):
        for sub in range(rows_chunk // 128):
            rows = slice(c * rows_chunk + sub * 128, c * rows_chunk + sub * 128 + 128)
            for g in range(2):
                value = logits(slot, g, rows)
                if tops is not None:
                    value = value - tops[g]
                parts[g] = parts[g] + jnp.sum(jnp.exp(value).reshape(16, 8, 128), axis=0)

    def close(slot, parts, tops, labels):
        for g in range(2):
            lse = jnp.log(jnp.sum(parts[g], axis=0, keepdims=True))
            if tops is not None:
                lse = lse + tops[g]
            lp_v[slot, g, 0:1, :] = logits(slot, g, slice(0, 1)) - lse
            lp_v[slot, g, 1:2, :] = labels[g] - lse

    def place(tile, slot):
        wide = []
        for g in range(2):
            turned = jnp.concatenate([jnp.broadcast_to(lp_v[slot, g, 0:1, :], (half, 128)),
                                      jnp.broadcast_to(lp_v[slot, g, 1:2, :], (half, 128))], axis=0).T
            wide += [turned[OCT * k:OCT * k + OCT, :] for k in range(16)]
        for k in range(items):
            row = pl.multiple_of(entry_of(tile, 3, k), OCT)
            here = lane_utt == entry_of(tile, 4, k)
            for j in range(n_oct):
                pltpu.store(both_d.at[pl.ds(row + OCT * j, OCT), :], wide[n_oct * k + j], mask=here)

    def matmul_chunk(slot, c):
        rows = slice(c * rows_chunk, (c + 1) * rows_chunk)
        z = lax.dot_general(w_t[rows, :], hid[slot], (((1,), (1,)), ((), ())), preferred_element_type=jnp.float32)
        for g in range(2):
            z_v[slot, g, rows, :] = z[:, 128 * g:128 * g + 128]

    def zeros():
        return [jnp.zeros((8, 128), jnp.float32) for _ in range(2)]

    def step(tile, slot, multiply=True, prepare=True):
        labels = [label_row(tile, slot, g) for g in range(2)]
        parts = zeros()
        for c in range(n_chunk):
            sum_chunk(slot, c, parts, None)
            if multiply:
                matmul_chunk(1 - slot, c)
            if prepare:
                hidden_chunk(tile + 2, slot, c)
        close(slot, parts, None, labels)

    n_tiles = (total + items - 1) // items
    hid[...] = jnp.zeros_like(hid)

    @pl.when((n_tiles > 0) & narrow)
    def _():
        for c in range(n_chunk):
            hidden_chunk(0, 0, c)
        for c in range(n_chunk):
            matmul_chunk(0, c)
            hidden_chunk(1, 1, c)

        def two_tiles(p, _):
            i = 2 * p
            place(jnp.maximum(i - 1, 1), 1)
            place(jnp.maximum(i - 2, 0), 0)
            step(i, 0)
            step(i + 1, 1)
            return 0

        n_pairs = (n_tiles - 1) // 2
        lax.fori_loop(0, n_pairs, two_tiles, 0)
        place(jnp.maximum(2 * n_pairs - 1, 1), 1)
        place(jnp.maximum(2 * n_pairs - 2, 0), 0)

        @pl.when(n_tiles % 2 == 0)
        def _():
            step(n_tiles - 2, 0, prepare=False)
            step(n_tiles - 1, 1, multiply=False, prepare=False)

        @pl.when(n_tiles % 2 == 1)
        def _():
            step(n_tiles - 1, 0, multiply=False, prepare=False)

        place(2 * n_pairs + 1, 1)
        place(2 * n_pairs, 0)

    @pl.when((n_tiles > 0) & jnp.logical_not(narrow))
    def _():
        def one_tile(i, _):
            for c in range(n_chunk):
                hidden_chunk(i, 0, c)
            for c in range(n_chunk):
                matmul_chunk(0, c)
            tops = []
            for g in range(2):
                top = jnp.full((8, 128), NEG_FILL, jnp.float32)
                for c in range(vocab // 128):
                    rows = slice(c * 128, c * 128 + 128)
                    top = jnp.maximum(top, jnp.max(logits(0, g, rows).reshape(16, 8, 128), axis=0))
                tops.append(jnp.max(top, axis=0, keepdims=True))
            labels = [label_row(i, 0, g) for g in range(2)]
            parts = zeros()
            for c in range(n_chunk):
                sum_chunk(0, c, parts, tops)
            close(0, parts, tops, labels)
            place(i, 0)
            return 0

        lax.fori_loop(0, n_tiles, one_tile, 0)

    flen = jnp.zeros((OCT, 128), jnp.int32)
    for b in range(n_utt):
        flen = jnp.where(lane_utt == b, flen_s[b] - t0, flen)
    for k in range(n_oct):
        live = k * OCT + frame8 < flen
        for u in range(n_pos):
            rows = slice(u * t_local + k * OCT, u * t_local + (k + 1) * OCT)
            both = both_d[rows, :]
            blank_d[rows, :] = jnp.where(live, both, 0.0)
            label_d[rows, :] = jnp.where(live, pltpu.roll(both, half, 1), NEG_FILL)

    entry = frame8 * rep + lane8 % rep
    stay = [jnp.where(entry == u, 0.0, NEG_FILL) for u in range(n_pos)]
    move = [None] * n_pos
    for d in range(t_local + n_pos - 1):
        for u in range(min(d, n_pos - 1), max(d - t_local, -1), -1):
            t = d - u
            row = u * t_local + t
            if u == 0:
                alpha = stay[0]
            else:
                high, low = jnp.maximum(stay[u], move[u - 1]), jnp.minimum(stay[u], move[u - 1])
                alpha = high + jnp.log(1.0 + jnp.exp(low - high))
            stay[u] = alpha + blank_d[row:row + 1, :]
            move[u] = alpha + label_d[row:row + 1, :]
    n_turn = n_pos // rep
    for u in range(n_pos):
        for j in range(n_turn):
            turn_v[j // 4, GROUP * (j % 4) + u:GROUP * (j % 4) + u + 1, :] = stay[u][j:j + 1, :]
    per = 128 // GROUP
    group = lane8 // GROUP
    lower = frame8 < rep
    turned = [turn_v[k].T[:half, :] for k in range(2)]
    shifted = {}
    for h in range(n_utt // per):
        for i in range(n_turn // 2):
            out = None
            for q in range(per):
                vreg = (per * h + q) // 2
                pieces = []
                for c in range(2):
                    j = 2 * i + c
                    key = (j // 4, vreg, (q - j) % 4, (q % 2) != c)
                    if key not in shifted:
                        piece = turned[key[0]][8 * vreg:8 * vreg + 8, :]
                        if key[2]:
                            piece = pltpu.roll(piece, GROUP * key[2], 1)
                        if key[3]:
                            piece = pltpu.roll(piece, rep, 0)
                        shifted[key] = piece
                    pieces.append(shifted[key])
                piece = jnp.where(lower, pieces[0], pieces[1])
                out = piece if out is None else jnp.where(group == q, piece, out)
            m_out[h, 8 * i:8 * i + 8, :] = out


def lattice_kernel(n_seq, m_hbm, llen_hbm, loss_ref,
                   m_recv, llen_s, v_out, v_recv, send_sem, recv_sem, out_sem, in_sem, own_sem):
    n_hand, n_pos = m_hbm.shape[:2]
    n_utt = llen_hbm.shape[0]
    per = 128 // GROUP
    me = lax.axis_index("seq")
    mine = me < n_hand
    my_hand = jnp.minimum(me, n_hand - 1)

    barrier = pltpu.get_barrier_semaphore()

    def greet(other):
        pl.semaphore_signal(barrier, inc=1, device_id={"seq": other}, device_id_type=MESH)

    @pl.when(mine)
    def _():
        for d in range(n_seq):
            @pl.when(me != d)
            def _():
                greet(d)

    own_len = pltpu.make_async_copy(llen_hbm, llen_s, own_sem.at[0])
    own_matrix = pltpu.make_async_copy(m_hbm.at[my_hand], m_recv.at[me], own_sem.at[1])

    @pl.when(mine)
    def _():
        own_len.start()
        own_matrix.start()

    pl.semaphore_wait(barrier, jnp.where(mine, n_hand - 1, n_hand))

    def send_matrix(h):
        return pltpu.make_async_remote_copy(
            src_ref=m_hbm.at[h], dst_ref=m_recv.at[me], send_sem=send_sem.at[h], recv_sem=recv_sem.at[me],
            device_id={"seq": h}, device_id_type=MESH)

    for h in range(n_hand):
        @pl.when(me != h)
        def _():
            send_matrix(h).start()

    def send_row(d):
        return pltpu.make_async_remote_copy(
            src_ref=v_out, dst_ref=v_recv.at[my_hand], send_sem=out_sem.at[d], recv_sem=in_sem.at[my_hand],
            device_id={"seq": d}, device_id_type=MESH)

    @pl.when(mine)
    def _():
        own_len.wait()
        own_matrix.wait()

        def arrived(src):
            @pl.when(src != me)
            def _():
                pltpu.make_async_remote_copy(
                    src_ref=m_hbm.at[0], dst_ref=m_recv.at[src], send_sem=send_sem.at[0], recv_sem=recv_sem.at[src],
                    device_id={"seq": src}, device_id_type=MESH).wait_recv()

        sub = lax.broadcasted_iota(jnp.int32, (n_pos, 128), 0)
        lane = lax.broadcasted_iota(jnp.int32, (n_pos, 128), 1)
        turn_idx = lane // GROUP * GROUP + sub

        def join(src, row):
            arrived(src)
            col = jnp.take_along_axis(jnp.broadcast_to(row, (n_pos, 128)), turn_idx, axis=1, mode="promise_in_bounds")
            terms = col + m_recv[src]
            top = jnp.max(terms, axis=0, keepdims=True)
            return top + jnp.log(jnp.sum(jnp.exp(terms - top), axis=0, keepdims=True))

        arrived(jnp.int32(0))
        row = m_recv[0, 0:1, :]
        row = lax.fori_loop(1, n_seq, join, row)
        sub8 = lax.broadcasted_iota(jnp.int32, (8, 128), 0)
        lane8 = lax.broadcasted_iota(jnp.int32, (8, 128), 1)
        want = jnp.full((8, 128), -1, jnp.int32)
        for b in range(n_utt):
            want = jnp.where(my_hand * per + sub8 == b, llen_s[b], want)
        keep = (lane8 // GROUP == sub8) & (lane8 % GROUP == want)
        column = jnp.sum(jnp.where(keep, row, 0.0), axis=1, keepdims=True)
        here = (lane8 == my_hand * per + sub8) & (sub8 < per)
        v_out[...] = jnp.sum(jnp.where(here, column, 0.0), axis=0, keepdims=True)
        for d in range(n_seq):
            @pl.when(me != d)
            def _():
                send_row(d).start()
        v_recv[my_hand] = v_out[...]

    for h in range(n_hand):
        @pl.when(me != h)
        def _():
            pltpu.make_async_remote_copy(
                src_ref=v_out, dst_ref=v_recv.at[h], send_sem=out_sem.at[0], recv_sem=in_sem.at[h],
                device_id={"seq": h}, device_id_type=MESH).wait_recv()
    total = v_recv[0]
    for h in range(1, n_hand):
        total = total + v_recv[h]
    loss_ref[...] = -total[0, :n_utt]

    for h in range(n_hand):
        @pl.when(me != h)
        def _():
            send_matrix(h).wait_send()

    @pl.when(mine)
    def _():
        for d in range(n_seq):
            @pl.when(me != d)
            def _():
                send_row(d).wait_send()


def joint_call(enc_blk, pred_out, w_enc, w_pred, w_out, b_out, labels, frame_len, label_len):
    n_utt, t_local, d_enc = enc_blk.shape
    n_pos, d_pred = pred_out.shape[1:]
    joint, vocab = w_out.shape
    n_slab = joint // 128
    per = 128 // GROUP
    items = TILE // t_local
    tab_rows = -(-(-(-n_utt * n_pos // items) + 3) // 8) * 8
    hbm = pl.BlockSpec(memory_space=pl.ANY)
    vmem = pl.BlockSpec(memory_space=pltpu.VMEM)
    f32, bf16, i32 = jnp.float32, jnp.bfloat16, jnp.int32
    return pl.pallas_call(
        joint_kernel,
        out_shape=pltpu.VMEM((n_utt // per, n_pos, 128), f32),
        in_specs=[hbm] * 9,
        out_specs=vmem,
        scratch_shapes=[
            pltpu.VMEM((n_utt * t_local, d_enc), bf16),
            pltpu.VMEM((n_utt * n_pos, d_pred), bf16),
            pltpu.VMEM((d_enc, joint), bf16),
            pltpu.VMEM((d_pred, joint), bf16),
            pltpu.VMEM((joint, vocab), bf16),
            pltpu.VMEM((vocab // 128, 128), f32),
            pltpu.VMEM((n_utt, n_pos - 1), i32),
            pltpu.VMEM((n_utt, 128), i32),
            pltpu.SMEM((n_utt,), i32),
            pltpu.SMEM((n_utt,), i32),
            pltpu.VMEM((vocab, joint), bf16),
            pltpu.VMEM((vocab + 8, 128), f32),
            pltpu.VMEM((n_slab, n_utt * t_local, 128), f32),
            pltpu.VMEM((n_slab, n_utt * n_pos, 128), f32),
            pltpu.VMEM((2, TILE, joint), bf16),
            pltpu.VMEM((2, 2, vocab + 8, 128), f32),
            pltpu.VMEM((2, 2, 8, 128), f32),
            pltpu.VMEM((t_local * n_pos, 128), f32),
            pltpu.VMEM((t_local * n_pos, 128), f32),
            pltpu.VMEM((t_local * n_pos, 128), f32),
            pltpu.VMEM((2, 128, 128), f32),
            pltpu.VMEM((tab_rows, 128), i32),
            pltpu.SMEM((tab_rows, 128), i32),
            pltpu.SemaphoreType.DMA((9,)),
            pltpu.SemaphoreType.DMA,
        ],

        name="joint",
    )(enc_blk.reshape(n_utt * t_local, d_enc), pred_out.reshape(n_utt * n_pos, d_pred), w_enc, w_pred, w_out,
      b_out.reshape(vocab // 128, 128), labels, frame_len, label_len)


def lattice_call(n_seq, matrices, label_len):
    n_hand, n_pos = matrices.shape[:2]
    n_utt = label_len.shape[0]
    f32 = jnp.float32
    return pl.pallas_call(
        functools.partial(lattice_kernel, n_seq),
        out_shape=pltpu.VMEM((n_utt,), f32),
        in_specs=[pl.BlockSpec(memory_space=pltpu.VMEM), pl.BlockSpec(memory_space=pl.ANY)],
        out_specs=pl.BlockSpec(memory_space=pltpu.VMEM),
        scratch_shapes=[
            pltpu.VMEM((n_seq, n_pos, 128), f32),
            pltpu.SMEM((n_utt,), jnp.int32),
            pltpu.VMEM((1, 128), f32),
            pltpu.VMEM((n_hand, 1, 128), f32),
            pltpu.SemaphoreType.DMA((n_hand,)),
            pltpu.SemaphoreType.DMA((n_seq,)),
            pltpu.SemaphoreType.DMA((n_seq,)),
            pltpu.SemaphoreType.DMA((n_hand,)),
            pltpu.SemaphoreType.DMA((2,)),
        ],
        compiler_params=pltpu.CompilerParams(collective_id=0, has_side_effects=True),
        name="lattice",
    )(matrices, label_len)


def solution(mesh):
    n_seq = mesh.shape["seq"]

    def local_loss(enc_blk, pred_out, w_enc, w_pred, w_out, b_out, labels, frame_len, label_len):
        matrices = joint_call(enc_blk, pred_out, w_enc, w_pred, w_out, b_out, labels, frame_len, label_len)
        return lattice_call(n_seq, pltpu.with_memory_space_constraint(matrices, pltpu.VMEM), label_len)

    in_specs = (P("dp", "seq", None), P("dp", None, None), P(), P(), P(), P(), P("dp", None), P("dp"), P("dp"))
    return jax.shard_map(local_loss, mesh=mesh, in_specs=in_specs, out_specs=P("dp"), check_vma=False)
```

```python
import functools
import jax
import jax.numpy as jnp
from jax import lax
from jax.experimental import pallas as pl
from jax.experimental.pallas import tpu as pltpu
from jax.sharding import PartitionSpec as P

NEG_FILL = -1.0e30
OCT = 8
TILE = 256
FIELD = 16
GROUP = 32
FIRST_HAND = 12
MESH = pl.DeviceIdType.MESH


def joint_kernel(enc_hbm, pred_hbm, wenc_hbm, wpred_hbm, wout_hbm, bout_hbm, lab_hbm, flen_hbm, llen_hbm,
                 m_out,
                 enc_v, pred_v, wenc_v, wpred_v, wout_v, bout_v, lab_raw, lab_v, flen_s, llen_s,
                 w_t, bias_t, a_v, c_v, hid, z_v, lp_v, both_d, blank_d, label_d, turn_v, tab_v, tab_s, sems, tab_sem):
    n_utt, n_lab = lab_hbm.shape
    n_pos = n_lab + 1
    t_local = enc_v.shape[0] // n_utt
    n_oct = t_local // OCT
    items = TILE // t_local
    joint, vocab = wout_v.shape
    n_slab = joint // 128
    half = 64
    rep = half // n_utt
    t0 = lax.axis_index("seq") * t_local

    copies = [
        pltpu.make_async_copy(src, dst, sems.at[k])
        for k, (src, dst) in enumerate([
            (flen_hbm, flen_s), (llen_hbm, llen_s), (lab_hbm, lab_raw), (bout_hbm, bout_v),
            (wout_hbm, wout_v), (enc_hbm, enc_v), (wenc_hbm, wenc_v), (pred_hbm, pred_v), (wpred_hbm, wpred_v)])
    ]
    for copy in copies:
        copy.start()

    both_d[...] = jnp.where(lax.broadcasted_iota(jnp.int32, both_d.shape, 1) < half, 0.0, NEG_FILL)

    for copy in copies[:3]:
        copy.wait()
    lab_v[...] = jnp.zeros_like(lab_v)
    lab_v[:, :n_lab] = lab_raw[...]
    shape = tab_v.shape
    cums, nus, total = [], [], jnp.int32(0)
    for b in range(n_utt):
        cums.append(total)
        nus.append(llen_s[b] + 1)
        total = total + jnp.where(flen_s[b] > t0, nus[b], 0)
    lane = lax.broadcasted_iota(jnp.int32, shape, 1)
    item = lax.broadcasted_iota(jnp.int32, shape, 0) * items + jnp.minimum(lane % FIELD, items - 1)
    item = jnp.minimum(item, total - 1)
    utt = jnp.zeros(shape, jnp.int32)
    base = jnp.zeros(shape, jnp.int32)
    width = jnp.ones(shape, jnp.int32)
    for b in range(n_utt):
        hit = item >= cums[b]
        utt = jnp.where(hit, b, utt)
        base = jnp.where(hit, cums[b], base)
        width = jnp.where(hit, nus[b], width)
    pos = jnp.clip(item - base, 0, n_pos - 1)
    word = jnp.zeros(shape, jnp.int32)
    for b in range(n_utt):
        row = jnp.broadcast_to(lab_v[b:b + 1, :], shape)
        word = jnp.where(utt == b, jnp.take_along_axis(row, pos, axis=1, mode="promise_in_bounds"), word)
    word = jnp.where(pos < width - 1, word, vocab)
    field = lane // FIELD
    tab_v[...] = jnp.where(field == 0, utt * t_local,
                           jnp.where(field == 1, utt * n_pos + pos,
                                     jnp.where(field == 2, word, jnp.where(field == 3, pos * t_local, utt))))
    tab_copy = pltpu.make_async_copy(tab_v, tab_s, tab_sem)
    tab_copy.start()

    copies[3].wait()
    copies[4].wait()
    top_bias = jnp.max(bout_v[...])
    bias_t[vocab:, :] = jnp.full((8, 128), NEG_FILL, jnp.float32)
    z_v[:, :, vocab:, :] = jnp.zeros((2, 2, 8, 128), jnp.float32)
    spread = jnp.zeros((8, 128), jnp.float32)
    for k in range(vocab // 128):
        cols = pl.ds(k * 128, 128)
        w_t[cols, :] = wout_v[:, cols].T
        bias_t[cols, :] = jnp.broadcast_to(bout_v[k:k + 1, :] - top_bias, (128, 128)).T
        mass = jnp.sum(jnp.abs(wout_v[:, cols].astype(jnp.float32)).reshape(joint // 8, 8, 128), axis=0)
        spread = jnp.maximum(spread, jnp.sum(mass, axis=0, keepdims=True))
    narrow = jnp.max(spread) <= 60.0
    copies[5].wait()
    copies[6].wait()
    proj = jnp.dot(enc_v[...], wenc_v[...], preferred_element_type=jnp.float32).astype(jnp.bfloat16).astype(jnp.float32)
    for s in range(n_slab):
        a_v[s] = proj[:, 128 * s:128 * s + 128]
    copies[7].wait()
    copies[8].wait()
    proj = jnp.dot(pred_v[...], wpred_v[...], preferred_element_type=jnp.float32).astype(jnp.bfloat16).astype(jnp.float32)
    for s in range(n_slab):
        c_v[s] = proj[:, 128 * s:128 * s + 128]
    tab_copy.wait()

    lane8 = lax.broadcasted_iota(jnp.int32, (OCT, 128), 1)
    frame8 = lax.broadcasted_iota(jnp.int32, (OCT, 128), 0)
    lane_utt = lane8 % half // rep
    lane_item = [(lax.broadcasted_iota(jnp.int32, (1, 128), 1) + 128 * g) // t_local for g in range(2)]
    n_chunk = 4
    rows_chunk = vocab // n_chunk

    def entry_of(tile, which, k):
        return tab_s[tile, FIELD * which + k]

    def hidden_chunk(tile, slot, c):
        for q in range(items // 2):
            if q * n_chunk // (items // 2) != c:
                continue
            pair = (2 * q, 2 * q + 1)
            a_rows = [pl.ds(pl.multiple_of(entry_of(tile, 0, k), OCT), t_local) for k in pair]
            c_rows = [pl.ds(entry_of(tile, 1, k), 1) for k in pair]
            rows = slice(2 * t_local * q, 2 * t_local * (q + 1))
            for s in range(n_slab):
                total_in = [a_v[s, a_row, :] + c_v[s, c_row, :] for a_row, c_row in zip(a_rows, c_rows)]
                hid[slot, rows, 128 * s:128 * s + 128] = jnp.tanh(
                    jnp.concatenate(total_in, axis=0)).astype(jnp.bfloat16)

    def logits(slot, g, rows):
        return z_v[slot, g, rows, :] + bias_t[rows, :]

    def label_row(tile, slot, g):
        value = jnp.zeros((1, 128), jnp.float32)
        for k in range(128 * g // t_local, min(items, (128 * g + 127) // t_local + 1)):
            value = jnp.where(lane_item[g] == k, logits(slot, g, pl.ds(entry_of(tile, 2, k), 1)), value)
        return value

    def sum_chunk(slot, c, parts, tops):
        for sub in range(rows_chunk // 128):
            rows = slice(c * rows_chunk + sub * 128, c * rows_chunk + sub * 128 + 128)
            for g in range(2):
                value = logits(slot, g, rows)
                if tops is not None:
                    value = value - tops[g]
                parts[g] = parts[g] + jnp.sum(jnp.exp(value).reshape(16, 8, 128), axis=0)

    def close(slot, parts, tops, labels):
        for g in range(2):
            lse = jnp.log(jnp.sum(parts[g], axis=0, keepdims=True))
            if tops is not None:
                lse = lse + tops[g]
            lp_v[slot, g, 0:1, :] = logits(slot, g, slice(0, 1)) - lse
            lp_v[slot, g, 1:2, :] = labels[g] - lse

    def place(tile, slot):
        wide = []
        for g in range(2):
            turned = jnp.concatenate([jnp.broadcast_to(lp_v[slot, g, 0:1, :], (half, 128)),
                                      jnp.broadcast_to(lp_v[slot, g, 1:2, :], (half, 128))], axis=0).T
            wide += [turned[OCT * k:OCT * k + OCT, :] for k in range(16)]
        for k in range(items):
            row = pl.multiple_of(entry_of(tile, 3, k), OCT)
            here = lane_utt == entry_of(tile, 4, k)
            for j in range(n_oct):
                pltpu.store(both_d.at[pl.ds(row + OCT * j, OCT), :], wide[n_oct * k + j], mask=here)

    def matmul_chunk(slot, c):
        rows = slice(c * rows_chunk, (c + 1) * rows_chunk)
        z = lax.dot_general(w_t[rows, :], hid[slot], (((1,), (1,)), ((), ())), preferred_element_type=jnp.float32)
        for g in range(2):
            z_v[slot, g, rows, :] = z[:, 128 * g:128 * g + 128]

    def zeros():
        return [jnp.zeros((8, 128), jnp.float32) for _ in range(2)]

    def step(tile, slot, multiply=True, prepare=True):
        labels = [label_row(tile, slot, g) for g in range(2)]
        parts = zeros()
        for c in range(n_chunk):
            sum_chunk(slot, c, parts, None)
            if multiply:
                matmul_chunk(1 - slot, c)
            if prepare:
                hidden_chunk(tile + 2, slot, c)
        close(slot, parts, None, labels)

    n_tiles = (total + items - 1) // items
    hid[...] = jnp.zeros_like(hid)

    @pl.when((n_tiles > 0) & narrow)
    def _():
        for c in range(n_chunk):
            hidden_chunk(0, 0, c)
        for c in range(n_chunk):
            matmul_chunk(0, c)
            hidden_chunk(1, 1, c)

        def two_tiles(p, _):
            i = 2 * p
            place(jnp.maximum(i - 1, 1), 1)
            place(jnp.maximum(i - 2, 0), 0)
            step(i, 0)
            step(i + 1, 1)
            return 0

        n_pairs = (n_tiles - 1) // 2
        lax.fori_loop(0, n_pairs, two_tiles, 0)
        place(jnp.maximum(2 * n_pairs - 1, 1), 1)
        place(jnp.maximum(2 * n_pairs - 2, 0), 0)

        @pl.when(n_tiles % 2 == 0)
        def _():
            step(n_tiles - 2, 0, prepare=False)
            step(n_tiles - 1, 1, multiply=False, prepare=False)

        @pl.when(n_tiles % 2 == 1)
        def _():
            step(n_tiles - 1, 0, multiply=False, prepare=False)

        place(2 * n_pairs + 1, 1)
        place(2 * n_pairs, 0)

    @pl.when((n_tiles > 0) & jnp.logical_not(narrow))
    def _():
        def one_tile(i, _):
            for c in range(n_chunk):
                hidden_chunk(i, 0, c)
            for c in range(n_chunk):
                matmul_chunk(0, c)
            tops = []
            for g in range(2):
                top = jnp.full((8, 128), NEG_FILL, jnp.float32)
                for c in range(vocab // 128):
                    rows = slice(c * 128, c * 128 + 128)
                    top = jnp.maximum(top, jnp.max(logits(0, g, rows).reshape(16, 8, 128), axis=0))
                tops.append(jnp.max(top, axis=0, keepdims=True))
            labels = [label_row(i, 0, g) for g in range(2)]
            parts = zeros()
            for c in range(n_chunk):
                sum_chunk(0, c, parts, tops)
            close(0, parts, tops, labels)
            place(i, 0)
            return 0

        lax.fori_loop(0, n_tiles, one_tile, 0)

    flen = jnp.zeros((OCT, 128), jnp.int32)
    for b in range(n_utt):
        flen = jnp.where(lane_utt == b, flen_s[b] - t0, flen)
    for k in range(n_oct):
        live = k * OCT + frame8 < flen
        for u in range(n_pos):
            rows = slice(u * t_local + k * OCT, u * t_local + (k + 1) * OCT)
            both = both_d[rows, :]
            blank_d[rows, :] = jnp.where(live, both, 0.0)
            label_d[rows, :] = jnp.where(live, pltpu.roll(both, half, 1), NEG_FILL)

    entry = frame8 * rep + lane8 % rep
    stay = [jnp.where(entry == u, 0.0, NEG_FILL) for u in range(n_pos)]
    move = [None] * n_pos
    for d in range(t_local + n_pos - 1):
        for u in range(min(d, n_pos - 1), max(d - t_local, -1), -1):
            t = d - u
            row = u * t_local + t
            if u == 0:
                alpha = stay[0]
            else:
                high, low = jnp.maximum(stay[u], move[u - 1]), jnp.minimum(stay[u], move[u - 1])
                alpha = high + jnp.log(1.0 + jnp.exp(low - high))
            stay[u] = alpha + blank_d[row:row + 1, :]
            move[u] = alpha + label_d[row:row + 1, :]
    n_turn = n_pos // rep
    for u in range(n_pos):
        for j in range(n_turn):
            turn_v[j // 4, GROUP * (j % 4) + u:GROUP * (j % 4) + u + 1, :] = stay[u][j:j + 1, :]
    per = 128 // GROUP
    group = lane8 // GROUP
    lower = frame8 < rep
    turned = [turn_v[k].T[:half, :] for k in range(2)]
    shifted = {}
    lane_u = lane8 % GROUP
    for h in range(n_utt // per):
        rows = []
        for i in range(n_turn // 2):
            out = None
            for q in range(per):
                vreg = (per * h + q) // 2
                pieces = []
                for c in range(2):
                    j = 2 * i + c
                    key = (j // 4, vreg, (GROUP * (q - j) - (16 if i == 2 else 0)) % 128, (q % 2) != c)
                    if key not in shifted:
                        piece = turned[key[0]][8 * vreg:8 * vreg + 8, :]
                        if key[2]:
                            piece = pltpu.roll(piece, key[2], 1)
                        if key[3]:
                            piece = pltpu.roll(piece, rep, 0)
                        shifted[key] = piece
                    pieces.append(shifted[key])
                piece = jnp.where(lower, pieces[0], pieces[1])
                out = piece if out is None else jnp.where(group == q, piece, out)
            rows.append(out)
        m_out[h, 0:8, :] = rows[0]
        m_out[h, 8:16, :] = jnp.where(lane_u < 8, rows[2], rows[1])


def lattice_kernel(n_seq, n_pos, m_hbm, llen_hbm, loss_ref,
                   m_recv, llen_s, v_out, v_recv, send_sem, recv_sem, out_sem, in_sem, own_sem):
    n_hand = m_hbm.shape[0]
    n_utt = llen_hbm.shape[0]
    per = 128 // GROUP
    me = lax.axis_index("seq")
    mine = (me >= FIRST_HAND) & (me < FIRST_HAND + n_hand)
    my_hand = jnp.clip(me - FIRST_HAND, 0, n_hand - 1)

    barrier = pltpu.get_barrier_semaphore()

    def greet(other):
        pl.semaphore_signal(barrier, inc=1, device_id={"seq": other}, device_id_type=MESH)

    @pl.when(mine)
    def _():
        for d in range(n_seq):
            @pl.when(me != d)
            def _():
                greet(d)

    own_len = pltpu.make_async_copy(llen_hbm, llen_s, own_sem.at[0])
    own_matrix = pltpu.make_async_copy(m_hbm.at[my_hand], m_recv.at[me], own_sem.at[1])

    @pl.when(mine)
    def _():
        own_len.start()
        own_matrix.start()

    pl.semaphore_wait(barrier, jnp.where(mine, n_hand - 1, n_hand))

    def send_matrix(h):
        return pltpu.make_async_remote_copy(
            src_ref=m_hbm.at[h], dst_ref=m_recv.at[me], send_sem=send_sem.at[h], recv_sem=recv_sem.at[me],
            device_id={"seq": FIRST_HAND + h}, device_id_type=MESH)

    for h in range(n_hand):
        @pl.when(me != FIRST_HAND + h)
        def _():
            send_matrix(h).start()

    def send_row(d):
        return pltpu.make_async_remote_copy(
            src_ref=v_out, dst_ref=v_recv.at[my_hand], send_sem=out_sem.at[d], recv_sem=in_sem.at[my_hand],
            device_id={"seq": d}, device_id_type=MESH)

    @pl.when(mine)
    def _():
        own_len.wait()
        own_matrix.wait()

        def arrived(src):
            @pl.when(src != me)
            def _():
                pltpu.make_async_remote_copy(
                    src_ref=m_hbm.at[0], dst_ref=m_recv.at[src], send_sem=send_sem.at[0], recv_sem=recv_sem.at[src],
                    device_id={"seq": src}, device_id_type=MESH).wait_recv()

        sub = lax.broadcasted_iota(jnp.int32, (n_pos, 128), 0)
        lane = lax.broadcasted_iota(jnp.int32, (n_pos, 128), 1)
        turn_idx = lane // GROUP * GROUP + sub
        lane_u = lane[:8, :] % GROUP

        def join(src, row):
            arrived(src)
            col = jnp.take_along_axis(jnp.broadcast_to(row, (n_pos, 128)), turn_idx, axis=1, mode="promise_in_bounds")
            late = m_recv[src, 8:16, :]
            matrix = jnp.concatenate([
                m_recv[src, 0:8, :], jnp.where(lane_u >= 8, late, NEG_FILL),
                jnp.where(lane_u >= 16, pltpu.roll(late, 16, 1), NEG_FILL)], axis=0)
            terms = col + matrix
            top = jnp.max(terms, axis=0, keepdims=True)
            return top + jnp.log(jnp.sum(jnp.exp(terms - top), axis=0, keepdims=True))

        arrived(jnp.int32(0))
        row = m_recv[0, 0:1, :]
        row = lax.fori_loop(1, n_seq, join, row)
        sub8 = lax.broadcasted_iota(jnp.int32, (8, 128), 0)
        lane8 = lax.broadcasted_iota(jnp.int32, (8, 128), 1)
        want = jnp.full((8, 128), -1, jnp.int32)
        for b in range(n_utt):
            want = jnp.where(my_hand * per + sub8 == b, llen_s[b], want)
        keep = (lane8 // GROUP == sub8) & (lane8 % GROUP == want)
        column = jnp.sum(jnp.where(keep, row, 0.0), axis=1, keepdims=True)
        here = (lane8 == my_hand * per + sub8) & (sub8 < per)
        v_out[...] = jnp.sum(jnp.where(here, column, 0.0), axis=0, keepdims=True)
        for d in range(n_seq):
            @pl.when(me != d)
            def _():
                send_row(d).start()
        v_recv[my_hand] = v_out[...]

    for h in range(n_hand):
        @pl.when(me != FIRST_HAND + h)
        def _():
            pltpu.make_async_remote_copy(
                src_ref=v_out, dst_ref=v_recv.at[h], send_sem=out_sem.at[0], recv_sem=in_sem.at[h],
                device_id={"seq": FIRST_HAND + h}, device_id_type=MESH).wait_recv()
    total = v_recv[0]
    for h in range(1, n_hand):
        total = total + v_recv[h]
    loss_ref[...] = -total[0, :n_utt]

    for h in range(n_hand):
        @pl.when(me != FIRST_HAND + h)
        def _():
            send_matrix(h).wait_send()

    @pl.when(mine)
    def _():
        for d in range(n_seq):
            @pl.when(me != d)
            def _():
                send_row(d).wait_send()


def joint_call(enc_blk, pred_out, w_enc, w_pred, w_out, b_out, labels, frame_len, label_len):
    n_utt, t_local, d_enc = enc_blk.shape
    n_pos, d_pred = pred_out.shape[1:]
    joint, vocab = w_out.shape
    n_slab = joint // 128
    per = 128 // GROUP
    items = TILE // t_local
    tab_rows = -(-(-(-n_utt * n_pos // items) + 3) // 8) * 8
    hbm = pl.BlockSpec(memory_space=pl.ANY)
    vmem = pl.BlockSpec(memory_space=pltpu.VMEM)
    f32, bf16, i32 = jnp.float32, jnp.bfloat16, jnp.int32
    return pl.pallas_call(
        joint_kernel,
        out_shape=pltpu.VMEM((n_utt // per, 16, 128), f32),
        in_specs=[hbm] * 9,
        out_specs=vmem,
        scratch_shapes=[
            pltpu.VMEM((n_utt * t_local, d_enc), bf16),
            pltpu.VMEM((n_utt * n_pos, d_pred), bf16),
            pltpu.VMEM((d_enc, joint), bf16),
            pltpu.VMEM((d_pred, joint), bf16),
            pltpu.VMEM((joint, vocab), bf16),
            pltpu.VMEM((vocab // 128, 128), f32),
            pltpu.VMEM((n_utt, n_pos - 1), i32),
            pltpu.VMEM((n_utt, 128), i32),
            pltpu.SMEM((n_utt,), i32),
            pltpu.SMEM((n_utt,), i32),
            pltpu.VMEM((vocab, joint), bf16),
            pltpu.VMEM((vocab + 8, 128), f32),
            pltpu.VMEM((n_slab, n_utt * t_local, 128), f32),
            pltpu.VMEM((n_slab, n_utt * n_pos, 128), f32),
            pltpu.VMEM((2, TILE, joint), bf16),
            pltpu.VMEM((2, 2, vocab + 8, 128), f32),
            pltpu.VMEM((2, 2, 8, 128), f32),
            pltpu.VMEM((t_local * n_pos, 128), f32),
            pltpu.VMEM((t_local * n_pos, 128), f32),
            pltpu.VMEM((t_local * n_pos, 128), f32),
            pltpu.VMEM((2, 128, 128), f32),
            pltpu.VMEM((tab_rows, 128), i32),
            pltpu.SMEM((tab_rows, 128), i32),
            pltpu.SemaphoreType.DMA((9,)),
            pltpu.SemaphoreType.DMA,
        ],

        name="joint",
    )(enc_blk.reshape(n_utt * t_local, d_enc), pred_out.reshape(n_utt * n_pos, d_pred), w_enc, w_pred, w_out,
      b_out.reshape(vocab // 128, 128), labels, frame_len, label_len)


def lattice_call(n_seq, n_pos, matrices, label_len):
    n_hand = matrices.shape[0]
    n_utt = label_len.shape[0]
    f32 = jnp.float32
    return pl.pallas_call(
        functools.partial(lattice_kernel, n_seq, n_pos),
        out_shape=pltpu.VMEM((n_utt,), f32),
        in_specs=[pl.BlockSpec(memory_space=pltpu.VMEM), pl.BlockSpec(memory_space=pl.ANY)],
        out_specs=pl.BlockSpec(memory_space=pltpu.VMEM),
        scratch_shapes=[
            pltpu.VMEM((n_seq, 16, 128), f32),
            pltpu.SMEM((n_utt,), jnp.int32),
            pltpu.VMEM((1, 128), f32),
            pltpu.VMEM((n_hand, 1, 128), f32),
            pltpu.SemaphoreType.DMA((n_hand,)),
            pltpu.SemaphoreType.DMA((n_seq,)),
            pltpu.SemaphoreType.DMA((n_seq,)),
            pltpu.SemaphoreType.DMA((n_hand,)),
            pltpu.SemaphoreType.DMA((2,)),
        ],
        compiler_params=pltpu.CompilerParams(collective_id=0, has_side_effects=True),
        name="lattice",
    )(matrices, label_len)


def solution(mesh):
    n_seq = mesh.shape["seq"]

    def local_loss(enc_blk, pred_out, w_enc, w_pred, w_out, b_out, labels, frame_len, label_len):
        matrices = joint_call(enc_blk, pred_out, w_enc, w_pred, w_out, b_out, labels, frame_len, label_len)
        return lattice_call(n_seq, pred_out.shape[1], pltpu.with_memory_space_constraint(matrices, pltpu.VMEM), label_len)

    in_specs = (P("dp", "seq", None), P("dp", None, None), P(), P(), P(), P(), P("dp", None), P("dp"), P("dp"))
    return jax.shard_map(local_loss, mesh=mesh, in_specs=in_specs, out_specs=P("dp"), check_vma=False)
```

```python
import functools
import jax
import jax.numpy as jnp
from jax import lax
from jax.experimental import pallas as pl
from jax.experimental.pallas import tpu as pltpu
from jax.sharding import PartitionSpec as P

NEG_FILL = -1.0e30
OCT = 8
TILE = 256
FIELD = 16
GROUP = 32
N_HAND = 2
MESH = pl.DeviceIdType.MESH


def joint_kernel(enc_hbm, pred_hbm, wenc_hbm, wpred_hbm, wout_hbm, bout_hbm, lab_hbm, flen_hbm, llen_hbm,
                 m_out,
                 enc_v, pred_v, wenc_v, wpred_v, wout_v, bout_v, lab_raw, lab_v, flen_s, llen_s,
                 w_t, bias_t, a_v, c_v, hid, z_v, lp_v, both_d, blank_d, label_d, turn_v, tab_v, tab_s, sems, tab_sem):
    n_utt, n_lab = lab_hbm.shape
    n_pos = n_lab + 1
    t_local = enc_v.shape[0] // n_utt
    n_oct = t_local // OCT
    items = TILE // t_local
    joint, vocab = wout_v.shape
    n_slab = joint // 128
    half = 64
    rep = half // n_utt
    t0 = lax.axis_index("seq") * t_local

    copies = [
        pltpu.make_async_copy(src, dst, sems.at[k])
        for k, (src, dst) in enumerate([
            (flen_hbm, flen_s), (llen_hbm, llen_s), (lab_hbm, lab_raw), (bout_hbm, bout_v),
            (wout_hbm, wout_v), (enc_hbm, enc_v), (wenc_hbm, wenc_v), (pred_hbm, pred_v), (wpred_hbm, wpred_v)])
    ]
    for copy in copies:
        copy.start()

    both_d[...] = jnp.where(lax.broadcasted_iota(jnp.int32, both_d.shape, 1) < half, 0.0, NEG_FILL)

    for copy in copies[:3]:
        copy.wait()
    lab_v[...] = jnp.zeros_like(lab_v)
    lab_v[:, :n_lab] = lab_raw[...]
    shape = tab_v.shape
    cums, nus, total = [], [], jnp.int32(0)
    for b in range(n_utt):
        cums.append(total)
        nus.append(llen_s[b] + 1)
        total = total + jnp.where(flen_s[b] > t0, nus[b], 0)
    lane = lax.broadcasted_iota(jnp.int32, shape, 1)
    item = lax.broadcasted_iota(jnp.int32, shape, 0) * items + jnp.minimum(lane % FIELD, items - 1)
    item = jnp.minimum(item, total - 1)
    utt = jnp.zeros(shape, jnp.int32)
    base = jnp.zeros(shape, jnp.int32)
    width = jnp.ones(shape, jnp.int32)
    for b in range(n_utt):
        hit = item >= cums[b]
        utt = jnp.where(hit, b, utt)
        base = jnp.where(hit, cums[b], base)
        width = jnp.where(hit, nus[b], width)
    pos = jnp.clip(item - base, 0, n_pos - 1)
    word = jnp.zeros(shape, jnp.int32)
    for b in range(n_utt):
        row = jnp.broadcast_to(lab_v[b:b + 1, :], shape)
        word = jnp.where(utt == b, jnp.take_along_axis(row, pos, axis=1, mode="promise_in_bounds"), word)
    word = jnp.where(pos < width - 1, word, vocab)
    field = lane // FIELD
    tab_v[...] = jnp.where(field == 0, utt * t_local,
                           jnp.where(field == 1, utt * n_pos + pos,
                                     jnp.where(field == 2, word, jnp.where(field == 3, pos * t_local, utt))))
    tab_copy = pltpu.make_async_copy(tab_v, tab_s, tab_sem)
    tab_copy.start()

    copies[3].wait()
    copies[4].wait()
    top_bias = jnp.max(bout_v[...])
    bias_t[vocab:, :] = jnp.full((8, 128), NEG_FILL, jnp.float32)
    z_v[:, :, vocab:, :] = jnp.zeros((2, 2, 8, 128), jnp.float32)
    spread = jnp.zeros((8, 128), jnp.float32)
    for k in range(vocab // 128):
        cols = pl.ds(k * 128, 128)
        w_t[cols, :] = wout_v[:, cols].T
        bias_t[cols, :] = jnp.broadcast_to(bout_v[k:k + 1, :] - top_bias, (128, 128)).T
        mass = jnp.sum(jnp.abs(wout_v[:, cols].astype(jnp.float32)).reshape(joint // 8, 8, 128), axis=0)
        spread = jnp.maximum(spread, jnp.sum(mass, axis=0, keepdims=True))
    narrow = jnp.max(spread) <= 60.0
    copies[5].wait()
    copies[6].wait()
    proj = jnp.dot(enc_v[...], wenc_v[...], preferred_element_type=jnp.float32).astype(jnp.bfloat16).astype(jnp.float32)
    for s in range(n_slab):
        a_v[s] = proj[:, 128 * s:128 * s + 128]
    copies[7].wait()
    copies[8].wait()
    proj = jnp.dot(pred_v[...], wpred_v[...], preferred_element_type=jnp.float32).astype(jnp.bfloat16).astype(jnp.float32)
    for s in range(n_slab):
        c_v[s] = proj[:, 128 * s:128 * s + 128]
    tab_copy.wait()

    lane8 = lax.broadcasted_iota(jnp.int32, (OCT, 128), 1)
    frame8 = lax.broadcasted_iota(jnp.int32, (OCT, 128), 0)
    lane_utt = lane8 % half // rep
    lane_item = [(lax.broadcasted_iota(jnp.int32, (1, 128), 1) + 128 * g) // t_local for g in range(2)]
    n_chunk = 4
    rows_chunk = vocab // n_chunk

    def entry_of(tile, which, k):
        return tab_s[tile, FIELD * which + k]

    def hidden_chunk(tile, slot, c):
        for q in range(items // 2):
            if q * n_chunk // (items // 2) != c:
                continue
            pair = (2 * q, 2 * q + 1)
            a_rows = [pl.ds(pl.multiple_of(entry_of(tile, 0, k), OCT), t_local) for k in pair]
            c_rows = [pl.ds(entry_of(tile, 1, k), 1) for k in pair]
            rows = slice(2 * t_local * q, 2 * t_local * (q + 1))
            for s in range(n_slab):
                total_in = [a_v[s, a_row, :] + c_v[s, c_row, :] for a_row, c_row in zip(a_rows, c_rows)]
                hid[slot, rows, 128 * s:128 * s + 128] = jnp.tanh(
                    jnp.concatenate(total_in, axis=0)).astype(jnp.bfloat16)

    def logits(slot, g, rows):
        return z_v[slot, g, rows, :] + bias_t[rows, :]

    def label_row(tile, slot, g):
        value = jnp.zeros((1, 128), jnp.float32)
        for k in range(128 * g // t_local, min(items, (128 * g + 127) // t_local + 1)):
            value = jnp.where(lane_item[g] == k, logits(slot, g, pl.ds(entry_of(tile, 2, k), 1)), value)
        return value

    def sum_chunk(slot, c, parts, tops):
        for sub in range(rows_chunk // 128):
            rows = slice(c * rows_chunk + sub * 128, c * rows_chunk + sub * 128 + 128)
            for g in range(2):
                value = logits(slot, g, rows)
                if tops is not None:
                    value = value - tops[g]
                parts[g] = parts[g] + jnp.sum(jnp.exp(value).reshape(16, 8, 128), axis=0)

    def close(slot, parts, tops, labels):
        for g in range(2):
            lse = jnp.log(jnp.sum(parts[g], axis=0, keepdims=True))
            if tops is not None:
                lse = lse + tops[g]
            lp_v[slot, g, 0:1, :] = logits(slot, g, slice(0, 1)) - lse
            lp_v[slot, g, 1:2, :] = labels[g] - lse

    def place(tile, slot):
        wide = []
        for g in range(2):
            turned = jnp.concatenate([jnp.broadcast_to(lp_v[slot, g, 0:1, :], (half, 128)),
                                      jnp.broadcast_to(lp_v[slot, g, 1:2, :], (half, 128))], axis=0).T
            wide += [turned[OCT * k:OCT * k + OCT, :] for k in range(16)]
        for k in range(items):
            row = pl.multiple_of(entry_of(tile, 3, k), OCT)
            here = lane_utt == entry_of(tile, 4, k)
            for j in range(n_oct):
                pltpu.store(both_d.at[pl.ds(row + OCT * j, OCT), :], wide[n_oct * k + j], mask=here)

    def matmul_chunk(slot, c):
        rows = slice(c * rows_chunk, (c + 1) * rows_chunk)
        z = lax.dot_general(w_t[rows, :], hid[slot], (((1,), (1,)), ((), ())), preferred_element_type=jnp.float32)
        for g in range(2):
            z_v[slot, g, rows, :] = z[:, 128 * g:128 * g + 128]

    def zeros():
        return [jnp.zeros((8, 128), jnp.float32) for _ in range(2)]

    def step(tile, slot, multiply=True, prepare=True):
        labels = [label_row(tile, slot, g) for g in range(2)]
        parts = zeros()
        for c in range(n_chunk):
            sum_chunk(slot, c, parts, None)
            if multiply:
                matmul_chunk(1 - slot, c)
            if prepare:
                hidden_chunk(tile + 2, slot, c)
        close(slot, parts, None, labels)

    n_tiles = (total + items - 1) // items
    hid[...] = jnp.zeros_like(hid)

    @pl.when((n_tiles > 0) & narrow)
    def _():
        for c in range(n_chunk):
            hidden_chunk(0, 0, c)
        for c in range(n_chunk):
            matmul_chunk(0, c)
            hidden_chunk(1, 1, c)

        def two_tiles(p, _):
            i = 2 * p
            place(jnp.maximum(i - 1, 1), 1)
            place(jnp.maximum(i - 2, 0), 0)
            step(i, 0)
            step(i + 1, 1)
            return 0

        n_pairs = (n_tiles - 1) // 2
        lax.fori_loop(0, n_pairs, two_tiles, 0)
        place(jnp.maximum(2 * n_pairs - 1, 1), 1)
        place(jnp.maximum(2 * n_pairs - 2, 0), 0)

        @pl.when(n_tiles % 2 == 0)
        def _():
            step(n_tiles - 2, 0, prepare=False)
            step(n_tiles - 1, 1, multiply=False, prepare=False)

        @pl.when(n_tiles % 2 == 1)
        def _():
            step(n_tiles - 1, 0, multiply=False, prepare=False)

        place(2 * n_pairs + 1, 1)
        place(2 * n_pairs, 0)

    @pl.when((n_tiles > 0) & jnp.logical_not(narrow))
    def _():
        def one_tile(i, _):
            for c in range(n_chunk):
                hidden_chunk(i, 0, c)
            for c in range(n_chunk):
                matmul_chunk(0, c)
            tops = []
            for g in range(2):
                top = jnp.full((8, 128), NEG_FILL, jnp.float32)
                for c in range(vocab // 128):
                    rows = slice(c * 128, c * 128 + 128)
                    top = jnp.maximum(top, jnp.max(logits(0, g, rows).reshape(16, 8, 128), axis=0))
                tops.append(jnp.max(top, axis=0, keepdims=True))
            labels = [label_row(i, 0, g) for g in range(2)]
            parts = zeros()
            for c in range(n_chunk):
                sum_chunk(0, c, parts, tops)
            close(0, parts, tops, labels)
            place(i, 0)
            return 0

        lax.fori_loop(0, n_tiles, one_tile, 0)

    flen = jnp.zeros((OCT, 128), jnp.int32)
    for b in range(n_utt):
        flen = jnp.where(lane_utt == b, flen_s[b] - t0, flen)
    for k in range(n_oct):
        live = k * OCT + frame8 < flen
        for u in range(n_pos):
            rows = slice(u * t_local + k * OCT, u * t_local + (k + 1) * OCT)
            both = both_d[rows, :]
            blank_d[rows, :] = jnp.where(live, both, 0.0)
            label_d[rows, :] = jnp.where(live, pltpu.roll(both, half, 1), NEG_FILL)

    entry = frame8 * rep + lane8 % rep
    stay = [jnp.where(entry == u, 0.0, NEG_FILL) for u in range(n_pos)]
    move = [None] * n_pos
    for d in range(t_local + n_pos - 1):
        for u in range(min(d, n_pos - 1), max(d - t_local, -1), -1):
            t = d - u
            row = u * t_local + t
            if u == 0:
                alpha = stay[0]
            else:
                high, low = jnp.maximum(stay[u], move[u - 1]), jnp.minimum(stay[u], move[u - 1])
                alpha = high + jnp.log(1.0 + jnp.exp(low - high))
            stay[u] = alpha + blank_d[row:row + 1, :]
            move[u] = alpha + label_d[row:row + 1, :]
    n_turn = n_pos // rep
    for u in range(n_pos):
        for j in range(n_turn):
            turn_v[j // 4, GROUP * (j % 4) + u:GROUP * (j % 4) + u + 1, :] = stay[u][j:j + 1, :]
    per = 128 // GROUP
    group = lane8 // GROUP
    lower = frame8 < rep
    turned = [turn_v[k].T[:half, :] for k in range(2)]
    shifted = {}
    lane_u = lane8 % GROUP
    for h in range(n_utt // per):
        rows = []
        for i in range(n_turn // 2):
            out = None
            for q in range(per):
                vreg = (per * h + q) // 2
                pieces = []
                for c in range(2):
                    j = 2 * i + c
                    key = (j // 4, vreg, (GROUP * (q - j) - (16 if i == 2 else 0)) % 128, (q % 2) != c)
                    if key not in shifted:
                        piece = turned[key[0]][8 * vreg:8 * vreg + 8, :]
                        if key[2]:
                            piece = pltpu.roll(piece, key[2], 1)
                        if key[3]:
                            piece = pltpu.roll(piece, rep, 0)
                        shifted[key] = piece
                    pieces.append(shifted[key])
                piece = jnp.where(lower, pieces[0], pieces[1])
                out = piece if out is None else jnp.where(group == q, piece, out)
            rows.append(out)
        m_out[h, 0:8, :] = rows[0]
        m_out[h, 8:16, :] = jnp.where(lane_u < 8, rows[2], rows[1])


def lattice_kernel(n_seq, n_pos, m_hbm, llen_hbm, loss_ref,
                   m_recv, llen_s, v_out, v_recv, send_sem, recv_sem, out_sem, in_sem, own_sem):
    n_hand = N_HAND
    n_part = m_hbm.shape[0] // n_hand
    n_utt = llen_hbm.shape[0]
    per = 128 // GROUP
    first_hand = n_seq - n_hand
    me = lax.axis_index("seq")
    mine = me >= first_hand
    my_hand = jnp.maximum(me - first_hand, 0)

    barrier = pltpu.get_barrier_semaphore()

    def greet(other):
        pl.semaphore_signal(barrier, inc=1, device_id={"seq": other}, device_id_type=MESH)

    @pl.when(mine)
    def _():
        for d in range(n_seq):
            @pl.when(me != d)
            def _():
                greet(d)

    own_len = pltpu.make_async_copy(llen_hbm, llen_s, own_sem.at[0])
    own_matrix = pltpu.make_async_copy(m_hbm.at[pl.ds(my_hand * n_part, n_part)], m_recv.at[me], own_sem.at[1])

    @pl.when(mine)
    def _():
        own_len.start()
        own_matrix.start()

    pl.semaphore_wait(barrier, jnp.where(mine, n_hand - 1, n_hand))

    def send_matrix(h):
        return pltpu.make_async_remote_copy(
            src_ref=m_hbm.at[pl.ds(h * n_part, n_part)], dst_ref=m_recv.at[me], send_sem=send_sem.at[h], recv_sem=recv_sem.at[me],
            device_id={"seq": first_hand + h}, device_id_type=MESH)

    for h in range(n_hand):
        @pl.when(me != first_hand + h)
        def _():
            send_matrix(h).start()

    def send_row(d):
        return pltpu.make_async_remote_copy(
            src_ref=v_out, dst_ref=v_recv.at[my_hand], send_sem=out_sem.at[d], recv_sem=in_sem.at[my_hand],
            device_id={"seq": d}, device_id_type=MESH)

    @pl.when(mine)
    def _():
        own_len.wait()
        own_matrix.wait()

        def arrived(src):
            @pl.when(src != me)
            def _():
                pltpu.make_async_remote_copy(
                    src_ref=m_hbm.at[pl.ds(0, n_part)], dst_ref=m_recv.at[src], send_sem=send_sem.at[0], recv_sem=recv_sem.at[src],
                    device_id={"seq": src}, device_id_type=MESH).wait_recv()

        sub8 = lax.broadcasted_iota(jnp.int32, (8, 128), 0)
        lane8 = lax.broadcasted_iota(jnp.int32, (8, 128), 1)
        lane_u = lane8 % GROUP
        group_lane = lane8 // GROUP * GROUP
        n_slab = n_pos // 8

        def unpack(src, part):
            late = m_recv[src, part, 8:16, :]
            return [m_recv[src, part, 0:8, :], jnp.where(lane_u >= 8, late, NEG_FILL),
                    jnp.where(lane_u >= 16, pltpu.roll(late, 16, 1), NEG_FILL)]

        def lanes_of(x, index):
            return jnp.take_along_axis(x, index, axis=1, mode="promise_in_bounds")

        def join(row, matrix):
            row = jnp.broadcast_to(row, (8, 128))
            terms = jnp.concatenate([lanes_of(row, group_lane + sub8 + 8 * i) + matrix[i] for i in range(n_slab)], axis=0)
            top = jnp.max(terms, axis=0, keepdims=True)
            return top + jnp.log(jnp.sum(jnp.exp(terms - top), axis=0, keepdims=True))

        def product(left, right):
            terms = [[] for _ in range(n_slab)]
            for u in range(n_pos):
                from_u = right[u // 8][u % 8:u % 8 + 1, :]
                for i in range(u // 8 + 1):
                    terms[i].append(lanes_of(left[i], group_lane + u) + from_u)
            out = []
            for values in terms:
                top = functools.reduce(jnp.maximum, values)
                out.append(top + jnp.log(functools.reduce(jnp.add, [jnp.exp(v - top) for v in values])))
            return out

        def right_step(k, carry):
            src = n_seq - 2 - k
            arrived(src)
            out = []
            for part in range(n_part):
                out += product(unpack(src, part), list(carry[n_slab * part:n_slab * (part + 1)]))
            return tuple(out)

        def left_step(src, rows):
            arrived(src)
            return tuple(join(rows[part], unpack(src, part)) for part in range(n_part))

        arrived(jnp.int32(n_seq - 1))
        right = []
        for part in range(n_part):
            right += unpack(n_seq - 1, part)
        right = lax.fori_loop(0, n_seq // 2 - 1, right_step, tuple(right))
        arrived(jnp.int32(0))
        rows = lax.fori_loop(1, n_seq // 2, left_step, tuple(m_recv[0, part, 0:1, :] for part in range(n_part)))
        picked = jnp.zeros((1, 128), jnp.float32)
        for part in range(n_part):
            row = join(rows[part], right[n_slab * part:n_slab * (part + 1)])
            utt = (my_hand * n_part + part) * per + sub8
            want = jnp.full((8, 128), -1, jnp.int32)
            for b in range(n_utt):
                want = jnp.where(utt == b, llen_s[b], want)
            keep = (lane8 // GROUP == sub8) & (lane_u == want)
            column = jnp.sum(jnp.where(keep, row, 0.0), axis=1, keepdims=True)
            here = (lane8 == utt) & (sub8 < per)
            picked = picked + jnp.sum(jnp.where(here, column, 0.0), axis=0, keepdims=True)
        v_out[...] = picked
        for d in range(n_seq):
            @pl.when(me != d)
            def _():
                send_row(d).start()
        v_recv[my_hand] = v_out[...]

    for h in range(n_hand):
        @pl.when(me != first_hand + h)
        def _():
            pltpu.make_async_remote_copy(
                src_ref=v_out, dst_ref=v_recv.at[h], send_sem=out_sem.at[0], recv_sem=in_sem.at[h],
                device_id={"seq": first_hand + h}, device_id_type=MESH).wait_recv()
    total = v_recv[0]
    for h in range(1, n_hand):
        total = total + v_recv[h]
    loss_ref[...] = -total[0, :n_utt]

    for h in range(n_hand):
        @pl.when(me != first_hand + h)
        def _():
            send_matrix(h).wait_send()

    @pl.when(mine)
    def _():
        for d in range(n_seq):
            @pl.when(me != d)
            def _():
                send_row(d).wait_send()


def joint_call(enc_blk, pred_out, w_enc, w_pred, w_out, b_out, labels, frame_len, label_len):
    n_utt, t_local, d_enc = enc_blk.shape
    n_pos, d_pred = pred_out.shape[1:]
    joint, vocab = w_out.shape
    n_slab = joint // 128
    per = 128 // GROUP
    items = TILE // t_local
    tab_rows = -(-(-(-n_utt * n_pos // items) + 3) // 8) * 8
    hbm = pl.BlockSpec(memory_space=pl.ANY)
    vmem = pl.BlockSpec(memory_space=pltpu.VMEM)
    f32, bf16, i32 = jnp.float32, jnp.bfloat16, jnp.int32
    return pl.pallas_call(
        joint_kernel,
        out_shape=pltpu.VMEM((n_utt // per, 16, 128), f32),
        in_specs=[hbm] * 9,
        out_specs=vmem,
        scratch_shapes=[
            pltpu.VMEM((n_utt * t_local, d_enc), bf16),
            pltpu.VMEM((n_utt * n_pos, d_pred), bf16),
            pltpu.VMEM((d_enc, joint), bf16),
            pltpu.VMEM((d_pred, joint), bf16),
            pltpu.VMEM((joint, vocab), bf16),
            pltpu.VMEM((vocab // 128, 128), f32),
            pltpu.VMEM((n_utt, n_pos - 1), i32),
            pltpu.VMEM((n_utt, 128), i32),
            pltpu.SMEM((n_utt,), i32),
            pltpu.SMEM((n_utt,), i32),
            pltpu.VMEM((vocab, joint), bf16),
            pltpu.VMEM((vocab + 8, 128), f32),
            pltpu.VMEM((n_slab, n_utt * t_local, 128), f32),
            pltpu.VMEM((n_slab, n_utt * n_pos, 128), f32),
            pltpu.VMEM((2, TILE, joint), bf16),
            pltpu.VMEM((2, 2, vocab + 8, 128), f32),
            pltpu.VMEM((2, 2, 8, 128), f32),
            pltpu.VMEM((t_local * n_pos, 128), f32),
            pltpu.VMEM((t_local * n_pos, 128), f32),
            pltpu.VMEM((t_local * n_pos, 128), f32),
            pltpu.VMEM((2, 128, 128), f32),
            pltpu.VMEM((tab_rows, 128), i32),
            pltpu.SMEM((tab_rows, 128), i32),
            pltpu.SemaphoreType.DMA((9,)),
            pltpu.SemaphoreType.DMA,
        ],

        name="joint",
    )(enc_blk.reshape(n_utt * t_local, d_enc), pred_out.reshape(n_utt * n_pos, d_pred), w_enc, w_pred, w_out,
      b_out.reshape(vocab // 128, 128), labels, frame_len, label_len)


def lattice_call(n_seq, n_pos, matrices, label_len):
    n_hand = N_HAND
    n_utt = label_len.shape[0]
    f32 = jnp.float32
    return pl.pallas_call(
        functools.partial(lattice_kernel, n_seq, n_pos),
        out_shape=pltpu.VMEM((n_utt,), f32),
        in_specs=[pl.BlockSpec(memory_space=pltpu.VMEM), pl.BlockSpec(memory_space=pl.ANY)],
        out_specs=pl.BlockSpec(memory_space=pltpu.VMEM),
        scratch_shapes=[
            pltpu.VMEM((n_seq, matrices.shape[0] // n_hand, 16, 128), f32),
            pltpu.SMEM((n_utt,), jnp.int32),
            pltpu.VMEM((1, 128), f32),
            pltpu.VMEM((n_hand, 1, 128), f32),
            pltpu.SemaphoreType.DMA((n_hand,)),
            pltpu.SemaphoreType.DMA((n_seq,)),
            pltpu.SemaphoreType.DMA((n_seq,)),
            pltpu.SemaphoreType.DMA((n_hand,)),
            pltpu.SemaphoreType.DMA((2,)),
        ],
        compiler_params=pltpu.CompilerParams(collective_id=0, has_side_effects=True),
        name="lattice",
    )(matrices, label_len)


def solution(mesh):
    n_seq = mesh.shape["seq"]

    def local_loss(enc_blk, pred_out, w_enc, w_pred, w_out, b_out, labels, frame_len, label_len):
        matrices = joint_call(enc_blk, pred_out, w_enc, w_pred, w_out, b_out, labels, frame_len, label_len)
        return lattice_call(n_seq, pred_out.shape[1], pltpu.with_memory_space_constraint(matrices, pltpu.VMEM), label_len)

    in_specs = (P("dp", "seq", None), P("dp", None, None), P(), P(), P(), P(), P("dp", None), P("dp"), P("dp"))
    return jax.shard_map(local_loss, mesh=mesh, in_specs=in_specs, out_specs=P("dp"), check_vma=False)
```

```python
import functools
import jax
import jax.numpy as jnp
from jax import lax
from jax.experimental import pallas as pl
from jax.experimental.pallas import tpu as pltpu
from jax.sharding import PartitionSpec as P

NEG_FILL = -1.0e30
OCT = 8
TILE = 256
FIELD = 16
GROUP = 32
N_HAND = 1
MESH = pl.DeviceIdType.MESH


def joint_kernel(enc_hbm, pred_hbm, wenc_hbm, wpred_hbm, wout_hbm, bout_hbm, lab_hbm, flen_hbm, llen_hbm,
                 m_out,
                 enc_v, pred_v, wenc_v, wpred_v, wout_v, bout_v, lab_raw, lab_v, flen_s, llen_s,
                 w_t, bias_t, a_v, c_v, hid, z_v, lp_v, both_d, blank_d, label_d, turn_v, tab_v, tab_s, sems, tab_sem):
    n_utt, n_lab = lab_hbm.shape
    n_pos = n_lab + 1
    t_local = enc_v.shape[0] // n_utt
    n_oct = t_local // OCT
    items = TILE // t_local
    joint, vocab = wout_v.shape
    n_slab = joint // 128
    half = 64
    rep = half // n_utt
    t0 = lax.axis_index("seq") * t_local

    copies = [
        pltpu.make_async_copy(src, dst, sems.at[k])
        for k, (src, dst) in enumerate([
            (flen_hbm, flen_s), (llen_hbm, llen_s), (lab_hbm, lab_raw), (bout_hbm, bout_v),
            (wout_hbm, wout_v), (enc_hbm, enc_v), (wenc_hbm, wenc_v), (pred_hbm, pred_v), (wpred_hbm, wpred_v)])
    ]
    for copy in copies:
        copy.start()

    both_d[...] = jnp.where(lax.broadcasted_iota(jnp.int32, both_d.shape, 1) < half, 0.0, NEG_FILL)

    for copy in copies[:3]:
        copy.wait()
    lab_v[...] = jnp.zeros_like(lab_v)
    lab_v[:, :n_lab] = lab_raw[...]
    shape = tab_v.shape
    cums, nus, total = [], [], jnp.int32(0)
    for b in range(n_utt):
        cums.append(total)
        nus.append(llen_s[b] + 1)
        total = total + jnp.where(flen_s[b] > t0, nus[b], 0)
    lane = lax.broadcasted_iota(jnp.int32, shape, 1)
    item = lax.broadcasted_iota(jnp.int32, shape, 0) * items + jnp.minimum(lane % FIELD, items - 1)
    item = jnp.minimum(item, total - 1)
    utt = jnp.zeros(shape, jnp.int32)
    base = jnp.zeros(shape, jnp.int32)
    width = jnp.ones(shape, jnp.int32)
    for b in range(n_utt):
        hit = item >= cums[b]
        utt = jnp.where(hit, b, utt)
        base = jnp.where(hit, cums[b], base)
        width = jnp.where(hit, nus[b], width)
    pos = jnp.clip(item - base, 0, n_pos - 1)
    word = jnp.zeros(shape, jnp.int32)
    for b in range(n_utt):
        row = jnp.broadcast_to(lab_v[b:b + 1, :], shape)
        word = jnp.where(utt == b, jnp.take_along_axis(row, pos, axis=1, mode="promise_in_bounds"), word)
    word = jnp.where(pos < width - 1, word, vocab)
    field = lane // FIELD
    tab_v[...] = jnp.where(field == 0, utt * t_local,
                           jnp.where(field == 1, utt * n_pos + pos,
                                     jnp.where(field == 2, word, jnp.where(field == 3, pos * t_local, utt))))
    tab_copy = pltpu.make_async_copy(tab_v, tab_s, tab_sem)
    tab_copy.start()

    copies[3].wait()
    copies[4].wait()
    top_bias = jnp.max(bout_v[...])
    bias_t[vocab:, :] = jnp.full((8, 128), NEG_FILL, jnp.float32)
    z_v[:, :, vocab:, :] = jnp.zeros((2, 2, 8, 128), jnp.float32)
    spread = jnp.zeros((8, 128), jnp.float32)
    for k in range(vocab // 128):
        cols = pl.ds(k * 128, 128)
        w_t[cols, :] = wout_v[:, cols].T
        bias_t[cols, :] = jnp.broadcast_to(bout_v[k:k + 1, :] - top_bias, (128, 128)).T
        mass = jnp.sum(jnp.abs(wout_v[:, cols].astype(jnp.float32)).reshape(joint // 8, 8, 128), axis=0)
        spread = jnp.maximum(spread, jnp.sum(mass, axis=0, keepdims=True))
    narrow = jnp.max(spread) <= 60.0
    copies[5].wait()
    copies[6].wait()
    proj = jnp.dot(enc_v[...], wenc_v[...], preferred_element_type=jnp.float32).astype(jnp.bfloat16).astype(jnp.float32)
    for s in range(n_slab):
        a_v[s] = proj[:, 128 * s:128 * s + 128]
    copies[7].wait()
    copies[8].wait()
    proj = jnp.dot(pred_v[...], wpred_v[...], preferred_element_type=jnp.float32).astype(jnp.bfloat16).astype(jnp.float32)
    for s in range(n_slab):
        c_v[s] = proj[:, 128 * s:128 * s + 128]
    tab_copy.wait()

    lane8 = lax.broadcasted_iota(jnp.int32, (OCT, 128), 1)
    frame8 = lax.broadcasted_iota(jnp.int32, (OCT, 128), 0)
    lane_utt = lane8 % half // rep
    lane_item = [(lax.broadcasted_iota(jnp.int32, (1, 128), 1) + 128 * g) // t_local for g in range(2)]
    n_chunk = 4
    rows_chunk = vocab // n_chunk

    def entry_of(tile, which, k):
        return tab_s[tile, FIELD * which + k]

    def hidden_chunk(tile, slot, c):
        for q in range(items // 2):
            if q * n_chunk // (items // 2) != c:
                continue
            pair = (2 * q, 2 * q + 1)
            a_rows = [pl.ds(pl.multiple_of(entry_of(tile, 0, k), OCT), t_local) for k in pair]
            c_rows = [pl.ds(entry_of(tile, 1, k), 1) for k in pair]
            rows = slice(2 * t_local * q, 2 * t_local * (q + 1))
            for s in range(n_slab):
                total_in = [a_v[s, a_row, :] + c_v[s, c_row, :] for a_row, c_row in zip(a_rows, c_rows)]
                hid[slot, rows, 128 * s:128 * s + 128] = jnp.tanh(
                    jnp.concatenate(total_in, axis=0)).astype(jnp.bfloat16)

    def logits(slot, g, rows):
        return z_v[slot, g, rows, :] + bias_t[rows, :]

    def label_row(tile, slot, g):
        value = jnp.zeros((1, 128), jnp.float32)
        for k in range(128 * g // t_local, min(items, (128 * g + 127) // t_local + 1)):
            value = jnp.where(lane_item[g] == k, logits(slot, g, pl.ds(entry_of(tile, 2, k), 1)), value)
        return value

    def sum_chunk(slot, c, parts, tops):
        for sub in range(rows_chunk // 128):
            rows = slice(c * rows_chunk + sub * 128, c * rows_chunk + sub * 128 + 128)
            for g in range(2):
                value = logits(slot, g, rows)
                if tops is not None:
                    value = value - tops[g]
                parts[g] = parts[g] + jnp.sum(jnp.exp(value).reshape(16, 8, 128), axis=0)

    def close(slot, parts, tops, labels):
        for g in range(2):
            lse = jnp.log(jnp.sum(parts[g], axis=0, keepdims=True))
            if tops is not None:
                lse = lse + tops[g]
            lp_v[slot, g, 0:1, :] = logits(slot, g, slice(0, 1)) - lse
            lp_v[slot, g, 1:2, :] = labels[g] - lse

    def place(tile, slot):
        wide = []
        for g in range(2):
            turned = jnp.concatenate([jnp.broadcast_to(lp_v[slot, g, 0:1, :], (half, 128)),
                                      jnp.broadcast_to(lp_v[slot, g, 1:2, :], (half, 128))], axis=0).T
            wide += [turned[OCT * k:OCT * k + OCT, :] for k in range(16)]
        for k in range(items):
            row = pl.multiple_of(entry_of(tile, 3, k), OCT)
            here = lane_utt == entry_of(tile, 4, k)
            for j in range(n_oct):
                pltpu.store(both_d.at[pl.ds(row + OCT * j, OCT), :], wide[n_oct * k + j], mask=here)

    def matmul_chunk(slot, c):
        rows = slice(c * rows_chunk, (c + 1) * rows_chunk)
        z = lax.dot_general(w_t[rows, :], hid[slot], (((1,), (1,)), ((), ())), preferred_element_type=jnp.float32)
        for g in range(2):
            z_v[slot, g, rows, :] = z[:, 128 * g:128 * g + 128]

    def zeros():
        return [jnp.zeros((8, 128), jnp.float32) for _ in range(2)]

    def step(tile, slot, multiply=True, prepare=True):
        labels = [label_row(tile, slot, g) for g in range(2)]
        parts = zeros()
        for c in range(n_chunk):
            sum_chunk(slot, c, parts, None)
            if multiply:
                matmul_chunk(1 - slot, c)
            if prepare:
                hidden_chunk(tile + 2, slot, c)
        close(slot, parts, None, labels)

    n_tiles = (total + items - 1) // items
    hid[...] = jnp.zeros_like(hid)

    @pl.when((n_tiles > 0) & narrow)
    def _():
        for c in range(n_chunk):
            hidden_chunk(0, 0, c)
        for c in range(n_chunk):
            matmul_chunk(0, c)
            hidden_chunk(1, 1, c)

        def two_tiles(p, _):
            i = 2 * p
            place(jnp.maximum(i - 1, 1), 1)
            place(jnp.maximum(i - 2, 0), 0)
            step(i, 0)
            step(i + 1, 1)
            return 0

        n_pairs = (n_tiles - 1) // 2
        lax.fori_loop(0, n_pairs, two_tiles, 0)
        place(jnp.maximum(2 * n_pairs - 1, 1), 1)
        place(jnp.maximum(2 * n_pairs - 2, 0), 0)

        @pl.when(n_tiles % 2 == 0)
        def _():
            step(n_tiles - 2, 0, prepare=False)
            step(n_tiles - 1, 1, multiply=False, prepare=False)

        @pl.when(n_tiles % 2 == 1)
        def _():
            step(n_tiles - 1, 0, multiply=False, prepare=False)

        place(2 * n_pairs + 1, 1)
        place(2 * n_pairs, 0)

    @pl.when((n_tiles > 0) & jnp.logical_not(narrow))
    def _():
        def one_tile(i, _):
            for c in range(n_chunk):
                hidden_chunk(i, 0, c)
            for c in range(n_chunk):
                matmul_chunk(0, c)
            tops = []
            for g in range(2):
                top = jnp.full((8, 128), NEG_FILL, jnp.float32)
                for c in range(vocab // 128):
                    rows = slice(c * 128, c * 128 + 128)
                    top = jnp.maximum(top, jnp.max(logits(0, g, rows).reshape(16, 8, 128), axis=0))
                tops.append(jnp.max(top, axis=0, keepdims=True))
            labels = [label_row(i, 0, g) for g in range(2)]
            parts = zeros()
            for c in range(n_chunk):
                sum_chunk(0, c, parts, tops)
            close(0, parts, tops, labels)
            place(i, 0)
            return 0

        lax.fori_loop(0, n_tiles, one_tile, 0)

    flen = jnp.zeros((OCT, 128), jnp.int32)
    for b in range(n_utt):
        flen = jnp.where(lane_utt == b, flen_s[b] - t0, flen)
    for k in range(n_oct):
        live = k * OCT + frame8 < flen
        for u in range(n_pos):
            rows = slice(u * t_local + k * OCT, u * t_local + (k + 1) * OCT)
            both = both_d[rows, :]
            blank_d[rows, :] = jnp.where(live, both, 0.0)
            label_d[rows, :] = jnp.where(live, pltpu.roll(both, half, 1), NEG_FILL)

    entry = frame8 * rep + lane8 % rep
    stay = [jnp.where(entry == u, 0.0, NEG_FILL) for u in range(n_pos)]
    move = [None] * n_pos
    for d in range(t_local + n_pos - 1):
        for u in range(min(d, n_pos - 1), max(d - t_local, -1), -1):
            t = d - u
            row = u * t_local + t
            if u == 0:
                alpha = stay[0]
            else:
                high, low = jnp.maximum(stay[u], move[u - 1]), jnp.minimum(stay[u], move[u - 1])
                alpha = high + jnp.log(1.0 + jnp.exp(low - high))
            stay[u] = alpha + blank_d[row:row + 1, :]
            move[u] = alpha + label_d[row:row + 1, :]
    n_turn = n_pos // rep
    for u in range(n_pos):
        for j in range(n_turn):
            turn_v[j // 4, GROUP * (j % 4) + u:GROUP * (j % 4) + u + 1, :] = stay[u][j:j + 1, :]
    per = 128 // GROUP
    group = lane8 // GROUP
    lower = frame8 < rep
    turned = [turn_v[k].T[:half, :] for k in range(2)]
    shifted = {}
    lane_u = lane8 % GROUP
    for h in range(n_utt // per):
        rows = []
        for i in range(n_turn // 2):
            out = None
            for q in range(per):
                vreg = (per * h + q) // 2
                pieces = []
                for c in range(2):
                    j = 2 * i + c
                    key = (j // 4, vreg, (GROUP * (q - j) - (16 if i == 2 else 0)) % 128, (q % 2) != c)
                    if key not in shifted:
                        piece = turned[key[0]][8 * vreg:8 * vreg + 8, :]
                        if key[2]:
                            piece = pltpu.roll(piece, key[2], 1)
                        if key[3]:
                            piece = pltpu.roll(piece, rep, 0)
                        shifted[key] = piece
                    pieces.append(shifted[key])
                piece = jnp.where(lower, pieces[0], pieces[1])
                out = piece if out is None else jnp.where(group == q, piece, out)
            rows.append(out)
        m_out[h, 0:8, :] = rows[0]
        m_out[h, 8:16, :] = jnp.where(lane_u < 8, rows[2], rows[1])


def lattice_kernel(n_seq, n_pos, m_hbm, llen_hbm, loss_ref,
                   m_recv, llen_s, v_out, v_recv, send_sem, recv_sem, out_sem, in_sem, own_sem):
    n_hand = N_HAND
    n_part = m_hbm.shape[0] // n_hand
    n_utt = llen_hbm.shape[0]
    per = 128 // GROUP
    first_hand = n_seq - n_hand
    me = lax.axis_index("seq")
    mine = me >= first_hand
    my_hand = jnp.maximum(me - first_hand, 0)

    barrier = pltpu.get_barrier_semaphore()

    def greet(other):
        pl.semaphore_signal(barrier, inc=1, device_id={"seq": other}, device_id_type=MESH)

    @pl.when(mine)
    def _():
        for d in range(n_seq):
            @pl.when(me != d)
            def _():
                greet(d)

    own_len = pltpu.make_async_copy(llen_hbm, llen_s, own_sem.at[0])
    own_matrix = pltpu.make_async_copy(m_hbm.at[pl.ds(my_hand * n_part, n_part)], m_recv.at[me], own_sem.at[1])

    @pl.when(mine)
    def _():
        own_len.start()
        own_matrix.start()

    @pl.when(jnp.logical_not(mine))
    def _():
        pl.semaphore_wait(barrier, n_hand)

    if n_hand > 1:
        @pl.when(mine)
        def _():
            pl.semaphore_wait(barrier, n_hand - 1)


    def send_matrix(h):
        return pltpu.make_async_remote_copy(
            src_ref=m_hbm.at[pl.ds(h * n_part, n_part)], dst_ref=m_recv.at[me], send_sem=send_sem.at[h], recv_sem=recv_sem.at[me],
            device_id={"seq": first_hand + h}, device_id_type=MESH)

    for h in range(n_hand):
        @pl.when(me != first_hand + h)
        def _():
            send_matrix(h).start()

    def send_row(d):
        return pltpu.make_async_remote_copy(
            src_ref=v_out, dst_ref=v_recv.at[my_hand], send_sem=out_sem.at[d], recv_sem=in_sem.at[my_hand],
            device_id={"seq": d}, device_id_type=MESH)

    @pl.when(mine)
    def _():
        own_len.wait()
        own_matrix.wait()

        def arrived(src):
            @pl.when(src != me)
            def _():
                pltpu.make_async_remote_copy(
                    src_ref=m_hbm.at[pl.ds(0, n_part)], dst_ref=m_recv.at[src], send_sem=send_sem.at[0], recv_sem=recv_sem.at[src],
                    device_id={"seq": src}, device_id_type=MESH).wait_recv()

        sub8 = lax.broadcasted_iota(jnp.int32, (8, 128), 0)
        lane8 = lax.broadcasted_iota(jnp.int32, (8, 128), 1)
        lane_u = lane8 % GROUP
        group_lane = lane8 // GROUP * GROUP
        n_slab = n_pos // 8

        def unpack(src, part):
            late = m_recv[src, part, 8:16, :]
            return [m_recv[src, part, 0:8, :], jnp.where(lane_u >= 8, late, NEG_FILL),
                    jnp.where(lane_u >= 16, pltpu.roll(late, 16, 1), NEG_FILL)]

        def lanes_of(x, index):
            return jnp.take_along_axis(x, index, axis=1, mode="promise_in_bounds")

        def join(row, matrix):
            row = jnp.broadcast_to(row, (8, 128))
            terms = jnp.concatenate([lanes_of(row, group_lane + sub8 + 8 * i) + matrix[i] for i in range(n_slab)], axis=0)
            top = jnp.max(terms, axis=0, keepdims=True)
            return top + jnp.log(jnp.sum(jnp.exp(terms - top), axis=0, keepdims=True))

        def product(left, right):
            terms = [[] for _ in range(n_slab)]
            for u in range(n_pos):
                from_u = right[u // 8][u % 8:u % 8 + 1, :]
                for i in range(u // 8 + 1):
                    terms[i].append(lanes_of(left[i], group_lane + u) + from_u)
            out = []
            for values in terms:
                top = functools.reduce(jnp.maximum, values)
                out.append(top + jnp.log(functools.reduce(jnp.add, [jnp.exp(v - top) for v in values])))
            return out

        def right_step(k, carry):
            src = n_seq - 2 - k
            arrived(src)
            out = []
            for part in range(n_part):
                out += product(unpack(src, part), list(carry[n_slab * part:n_slab * (part + 1)]))
            return tuple(out)

        def left_step(src, rows):
            arrived(src)
            return tuple(join(rows[part], unpack(src, part)) for part in range(n_part))

        arrived(jnp.int32(n_seq - 1))
        right = []
        for part in range(n_part):
            right += unpack(n_seq - 1, part)
        right = lax.fori_loop(0, n_seq // 2 - 1, right_step, tuple(right))
        arrived(jnp.int32(0))
        rows = lax.fori_loop(1, n_seq // 2, left_step, tuple(m_recv[0, part, 0:1, :] for part in range(n_part)))
        picked = jnp.zeros((1, 128), jnp.float32)
        for part in range(n_part):
            row = join(rows[part], right[n_slab * part:n_slab * (part + 1)])
            utt = (my_hand * n_part + part) * per + sub8
            want = jnp.full((8, 128), -1, jnp.int32)
            for b in range(n_utt):
                want = jnp.where(utt == b, llen_s[b], want)
            keep = (lane8 // GROUP == sub8) & (lane_u == want)
            column = jnp.sum(jnp.where(keep, row, 0.0), axis=1, keepdims=True)
            here = (lane8 == utt) & (sub8 < per)
            picked = picked + jnp.sum(jnp.where(here, column, 0.0), axis=0, keepdims=True)
        v_out[...] = picked
        for d in range(n_seq):
            @pl.when(me != d)
            def _():
                send_row(d).start()
        v_recv[my_hand] = v_out[...]

    for h in range(n_hand):
        @pl.when(me != first_hand + h)
        def _():
            pltpu.make_async_remote_copy(
                src_ref=v_out, dst_ref=v_recv.at[h], send_sem=out_sem.at[0], recv_sem=in_sem.at[h],
                device_id={"seq": first_hand + h}, device_id_type=MESH).wait_recv()
    total = v_recv[0]
    for h in range(1, n_hand):
        total = total + v_recv[h]
    loss_ref[...] = -total[0, :n_utt]

    for h in range(n_hand):
        @pl.when(me != first_hand + h)
        def _():
            send_matrix(h).wait_send()

    @pl.when(mine)
    def _():
        for d in range(n_seq):
            @pl.when(me != d)
            def _():
                send_row(d).wait_send()


def joint_call(enc_blk, pred_out, w_enc, w_pred, w_out, b_out, labels, frame_len, label_len):
    n_utt, t_local, d_enc = enc_blk.shape
    n_pos, d_pred = pred_out.shape[1:]
    joint, vocab = w_out.shape
    n_slab = joint // 128
    per = 128 // GROUP
    items = TILE // t_local
    tab_rows = -(-(-(-n_utt * n_pos // items) + 3) // 8) * 8
    hbm = pl.BlockSpec(memory_space=pl.ANY)
    vmem = pl.BlockSpec(memory_space=pltpu.VMEM)
    f32, bf16, i32 = jnp.float32, jnp.bfloat16, jnp.int32
    return pl.pallas_call(
        joint_kernel,
        out_shape=pltpu.VMEM((n_utt // per, 16, 128), f32),
        in_specs=[hbm] * 9,
        out_specs=vmem,
        scratch_shapes=[
            pltpu.VMEM((n_utt * t_local, d_enc), bf16),
            pltpu.VMEM((n_utt * n_pos, d_pred), bf16),
            pltpu.VMEM((d_enc, joint), bf16),
            pltpu.VMEM((d_pred, joint), bf16),
            pltpu.VMEM((joint, vocab), bf16),
            pltpu.VMEM((vocab // 128, 128), f32),
            pltpu.VMEM((n_utt, n_pos - 1), i32),
            pltpu.VMEM((n_utt, 128), i32),
            pltpu.SMEM((n_utt,), i32),
            pltpu.SMEM((n_utt,), i32),
            pltpu.VMEM((vocab, joint), bf16),
            pltpu.VMEM((vocab + 8, 128), f32),
            pltpu.VMEM((n_slab, n_utt * t_local, 128), f32),
            pltpu.VMEM((n_slab, n_utt * n_pos, 128), f32),
            pltpu.VMEM((2, TILE, joint), bf16),
            pltpu.VMEM((2, 2, vocab + 8, 128), f32),
            pltpu.VMEM((2, 2, 8, 128), f32),
            pltpu.VMEM((t_local * n_pos, 128), f32),
            pltpu.VMEM((t_local * n_pos, 128), f32),
            pltpu.VMEM((t_local * n_pos, 128), f32),
            pltpu.VMEM((2, 128, 128), f32),
            pltpu.VMEM((tab_rows, 128), i32),
            pltpu.SMEM((tab_rows, 128), i32),
            pltpu.SemaphoreType.DMA((9,)),
            pltpu.SemaphoreType.DMA,
        ],

        name="joint",
    )(enc_blk.reshape(n_utt * t_local, d_enc), pred_out.reshape(n_utt * n_pos, d_pred), w_enc, w_pred, w_out,
      b_out.reshape(vocab // 128, 128), labels, frame_len, label_len)


def lattice_call(n_seq, n_pos, matrices, label_len):
    n_hand = N_HAND
    n_utt = label_len.shape[0]
    f32 = jnp.float32
    return pl.pallas_call(
        functools.partial(lattice_kernel, n_seq, n_pos),
        out_shape=pltpu.VMEM((n_utt,), f32),
        in_specs=[pl.BlockSpec(memory_space=pltpu.VMEM), pl.BlockSpec(memory_space=pl.ANY)],
        out_specs=pl.BlockSpec(memory_space=pltpu.VMEM),
        scratch_shapes=[
            pltpu.VMEM((n_seq, matrices.shape[0] // n_hand, 16, 128), f32),
            pltpu.SMEM((n_utt,), jnp.int32),
            pltpu.VMEM((1, 128), f32),
            pltpu.VMEM((n_hand, 1, 128), f32),
            pltpu.SemaphoreType.DMA((n_hand,)),
            pltpu.SemaphoreType.DMA((n_seq,)),
            pltpu.SemaphoreType.DMA((n_seq,)),
            pltpu.SemaphoreType.DMA((n_hand,)),
            pltpu.SemaphoreType.DMA((2,)),
        ],
        compiler_params=pltpu.CompilerParams(collective_id=0, has_side_effects=True),
        name="lattice",
    )(matrices, label_len)


def solution(mesh):
    n_seq = mesh.shape["seq"]

    def local_loss(enc_blk, pred_out, w_enc, w_pred, w_out, b_out, labels, frame_len, label_len):
        matrices = joint_call(enc_blk, pred_out, w_enc, w_pred, w_out, b_out, labels, frame_len, label_len)
        return lattice_call(n_seq, pred_out.shape[1], pltpu.with_memory_space_constraint(matrices, pltpu.VMEM), label_len)

    in_specs = (P("dp", "seq", None), P("dp", None, None), P(), P(), P(), P(), P("dp", None), P("dp"), P("dp"))
    return jax.shard_map(local_loss, mesh=mesh, in_specs=in_specs, out_specs=P("dp"), check_vma=False)
```
